512 devices in a mesh: seq: 64 (over x, y, z_hi), head: 8 (over z_lo, core).
Axes of the slice: x: 4, y: 8, z: 8 (z_hi: 2, z_lo: 4; z = z_hi * 4 + z_lo), core: 2. Of those that a mesh axis runs over, the one named last changes fastest.
Arguments:
- queries: bfloat16 [65536, 5120], P(('seq', 'head')), may hold values from -7.5 to 7.5
- keys: bfloat16 [65536, 1024], P(('seq', 'head')), may hold values from -7.5 to 7.5
- values: bfloat16 [65536, 1024], P(('seq', 'head')), may hold values from -6 to 6
- fetch_list: int32 [64, 64, 2], replicated, may hold values from 0 to 15, as said below
- choose: int32 [1024, 16], P('seq'), may hold values from 0 to 127, as said below
- live: int32 [1024], P('seq'), may hold values from 0 to 16, as said below
Outputs:
- attn_out: bfloat16 [65536, 5120], P(('seq', 'head'))
The draws below stay inside these ranges and needn't reach their ends.
Inputs may be any that keep to these rules, and one draw needn't show every extreme that they name: Each row fetch_list[d, s] holds 2 distinct blocks. Each row of choose holds 16 distinct slots; slot j stands for entry j % 2 of fetch_list[d, j // 2]; the first live[b] entries of row b name slots j with j // 2 < b // 16. live[b] is at most 2 * (b // 16); every draw has a block with live equal to 16.
All inputs are finite; a program needn't handle non-finite values.
Results may differ from the reference program's by a relative error of at most 0.0042.
Values may be sent and summed in bfloat16 or wider, within the bound.
A program may use at most 64 MiB of HBM per device.

```python
import math
import jax
import jax.numpy as jnp
from jax import lax

QUERY_HEADS = 40
KEY_VALUE_HEADS = 8
HEAD_WIDTH = 128
BLOCK_TOKENS = 64
CAP = 2
LISTED_ENTRIES = 16
TOK_DEV = 1024
CONTEXT_TOKENS = 65536
FILE_BLOCKS = 1024
SLOTS = 128
N_SEQ = 64


def draw_keys(key, part):
    filled_slots = jax.random.normal(jax.random.fold_in(key, 11), (CONTEXT_TOKENS, KEY_VALUE_HEADS * HEAD_WIDTH), jnp.float32)
    return jnp.clip(filled_slots, -7.5, 7.5).astype(jnp.bfloat16)


def draw_queries(key, part):
    filled_slots = jax.random.normal(jax.random.fold_in(key, 12), (CONTEXT_TOKENS, QUERY_HEADS * HEAD_WIDTH), jnp.float32)
    return jnp.clip(filled_slots, -7.5, 7.5).astype(jnp.bfloat16)


def draw_fetch_list(key, part):
    blocks_per_dev = TOK_DEV // BLOCK_TOKENS
    ranking = jax.random.randint(jax.random.fold_in(key, 21), (N_SEQ, N_SEQ, blocks_per_dev), 0, 1 << 20)
    ranking = ranking * blocks_per_dev + jnp.arange(blocks_per_dev, dtype=jnp.int32)
    return lax.top_k(ranking, CAP)[1].astype(jnp.int32)


def draw_choose(key, part):
    blocks_per_dev = TOK_DEV // BLOCK_TOKENS
    ranking = jax.random.randint(jax.random.fold_in(key, 22), (FILE_BLOCKS, SLOTS), 0, 1 << 16)
    ranking = ranking * SLOTS + jnp.arange(SLOTS, dtype=jnp.int32)
    shard_of = jnp.arange(FILE_BLOCKS, dtype=jnp.int32) // blocks_per_dev
    earlier = (jnp.arange(SLOTS, dtype=jnp.int32) // CAP)[None, :] < shard_of[:, None]
    ranking = ranking + earlier.astype(jnp.int32) * (1 << 24)
    return lax.top_k(ranking, LISTED_ENTRIES)[1].astype(jnp.int32)


def draw_live(key, part):
    blocks_per_dev = TOK_DEV // BLOCK_TOKENS
    heavy_share = jax.random.randint(jax.random.fold_in(key, 31), (N_SEQ,), 0, 6)
    heavy_roll = jax.random.randint(jax.random.fold_in(key, 32), (FILE_BLOCKS,), 0, 16)
    heavy = heavy_roll < jnp.repeat(heavy_share, FILE_BLOCKS // N_SEQ, total_repeat_length=FILE_BLOCKS)
    light_count = jax.random.randint(jax.random.fold_in(key, 33), (FILE_BLOCKS,), 1, 4)
    heavy_count = jax.random.randint(jax.random.fold_in(key, 34), (FILE_BLOCKS,), LISTED_ENTRIES // 2, LISTED_ENTRIES + 1)
    forced = (N_SEQ - 1) * blocks_per_dev + jax.random.randint(jax.random.fold_in(key, 35), (), 0, blocks_per_dev)
    counts = jnp.where(heavy, heavy_count, light_count)
    limit = CAP * (jnp.arange(FILE_BLOCKS, dtype=jnp.int32) // blocks_per_dev)
    counts = jnp.minimum(counts, limit)
    counts = jnp.where(jnp.arange(FILE_BLOCKS) == forced, LISTED_ENTRIES, counts)
    return counts.astype(jnp.int32)


def block_scale(key, extent, shards, smallest, largest):
    factor_of = 1.0
    for axis_at, shards_of in shards:
        heights = jax.random.uniform(jax.random.fold_in(jax.random.fold_in(key, 6), axis_at), (shards_of,), jnp.float32, smallest / len(shards), largest / len(shards))
        factor_of = factor_of * jnp.repeat(jnp.exp(heights), extent[axis_at] // shards_of).reshape((-1,) + (1,) * (len(extent) - 1 - axis_at))
    return factor_of


def gaussian(own_key, dims, scale, most, pieces=(), kind=jnp.bfloat16):
    entries = scale * jax.random.normal(own_key, dims, jnp.float32)
    if pieces:
        entries = entries * block_scale(own_key, dims, pieces, -0.22, 0.18)
    return jnp.clip(entries, -most, most).astype(kind)


def setup_inputs(seed: int = 0) -> dict:
    streams_of = jax.random.split(jax.random.key(seed), 7)
    return {
        "queries": draw_queries(jax.random.fold_in(streams_of[6], 71), 0),
        "keys": draw_keys(jax.random.fold_in(streams_of[6], 71), 0),
        "values": gaussian(streams_of[2], (CONTEXT_TOKENS, KEY_VALUE_HEADS * HEAD_WIDTH), 1.0, 6.0, ((0, 512),)),
        "fetch_list": draw_fetch_list(jax.random.fold_in(streams_of[6], 71), 0),
        "choose": draw_choose(jax.random.fold_in(streams_of[6], 71), 0),
        "live": draw_live(jax.random.fold_in(streams_of[6], 71), 0),
    }


def reference(queries, keys, values, fetch_list, choose, live):
    blocks_per_dev = TOK_DEV // BLOCK_TOKENS
    repeat_factor = QUERY_HEADS // KEY_VALUE_HEADS
    scaling = 1.0 / math.sqrt(HEAD_WIDTH)
    query_block_rows = queries.reshape(FILE_BLOCKS, BLOCK_TOKENS, KEY_VALUE_HEADS, repeat_factor, HEAD_WIDTH)
    key_block_rows = keys.reshape(FILE_BLOCKS, BLOCK_TOKENS, KEY_VALUE_HEADS, HEAD_WIDTH)
    value_block_rows = values.reshape(FILE_BLOCKS, BLOCK_TOKENS, KEY_VALUE_HEADS, HEAD_WIDTH)
    column = jnp.arange((LISTED_ENTRIES + 1) * BLOCK_TOKENS, dtype=jnp.int32)
    query_row = jnp.arange(BLOCK_TOKENS, dtype=jnp.int32)
    key_block = column // BLOCK_TOKENS

    def one_block(block_index):
        owner_dev = block_index // blocks_per_dev
        picked = choose[block_index]
        source = picked // CAP
        entry_slot = picked % CAP
        local_block = fetch_list[owner_dev, source, entry_slot]
        listed_entries = jnp.concatenate([block_index[None].astype(jnp.int32), (source * blocks_per_dev + local_block).astype(jnp.int32)])
        selected_keys = key_block_rows[listed_entries].reshape((LISTED_ENTRIES + 1) * BLOCK_TOKENS, KEY_VALUE_HEADS, HEAD_WIDTH).astype(jnp.float32)
        selected_values = value_block_rows[listed_entries].reshape((LISTED_ENTRIES + 1) * BLOCK_TOKENS, KEY_VALUE_HEADS, HEAD_WIDTH).astype(jnp.float32)
        query_part = query_block_rows[block_index].astype(jnp.float32)
        scores = jnp.einsum('qhgd,khd->hgqk', query_part, selected_keys) * scaling
        own_ok = (key_block == 0)[None, :] & (column[None, :] <= query_row[:, None])
        import_ok = ((key_block >= 1) & (key_block <= live[block_index]))[None, :]
        allowed = own_ok | import_ok
        scores = jnp.where(allowed[None, None], scores, -jnp.inf)
        highest = lax.optimization_barrier(jnp.max(scores, axis=-1, keepdims=True))
        weights = jnp.exp(scores - highest)
        totals = lax.optimization_barrier(jnp.sum(weights, axis=-1))
        rounded = lax.optimization_barrier(weights.astype(jnp.bfloat16)).astype(jnp.float32)
        mixed = jnp.einsum('hgqk,khd->qhgd', rounded, selected_values)
        result = mixed / jnp.transpose(totals, (2, 0, 1))[..., None]
        return result.astype(jnp.bfloat16).reshape(BLOCK_TOKENS, QUERY_HEADS * HEAD_WIDTH)
    outputs = lax.map(one_block, jnp.arange(FILE_BLOCKS, dtype=jnp.int32))
    return outputs.reshape(CONTEXT_TOKENS, QUERY_HEADS * HEAD_WIDTH)
```

```python
import functools
import math

import jax
import jax.numpy as jnp
from jax import lax
from jax.experimental import pallas as pl
from jax.experimental.pallas import tpu as pltpu
from jax.sharding import PartitionSpec as P

MESH = pl.DeviceIdType.MESH
WIDTH = 128
BLOCK = 64
ENTRIES = 16
X, Y, Z = 4, 8, 2
PLANE = Y * Z
GROUP = 8
REPEAT = 5
ROWS = 128
TOKENS = GROUP * ROWS
BLOCKS = TOKENS // BLOCK
QW = REPEAT * WIDTH
SCALE = math.log2(math.e) / math.sqrt(WIDTH)


def mirrored(z, i):
    return i + z * (6 + 2 * lax.rem(i, 2) - 2 * i)


def xor3(a, b):
    out = 0
    for bit in (4, 2, 1):
        out = out + bit * lax.rem(lax.rem(a // bit, 2) + lax.rem(b // bit, 2), 2)
    return out


def place(g, t):
    return t if g == 0 or t in (0, Y // 2) else Y // 2 + t


def kernel(
    fetch, choose, live, q_in, k_in, v_in, o_out,
    q_all, out_buf, items_k, items_v, pick_k, pick_v, got_k, got_v,
    q_send, q_recv, k_send, k_recv, v_send, v_recv,
    z_send, z_recv, y_send, y_recv, x_send, x_recv, o_send, o_recv, local_sem,
):
    s = lax.axis_index("seq")
    i = lax.axis_index("head")
    x, y, z = s // PLANE, lax.rem(s // Z, Y), lax.rem(s, Z)
    h = mirrored(z, i)
    own_k, own_v = items_k[0], items_v[0]
    picks = (pick_k, pick_v)
    gots = (got_k, got_v)

    def seq_of(ax, ay, az):
        return (ax * Y + ay) * Z + az

    right = (seq_of(x, lax.rem(y + 1, Y), z), i)
    left = (seq_of(x, lax.rem(y + Y - 1, Y), z), i)
    across = (seq_of(x, y, 1 - z), mirrored(1 - z, h))

    barrier = pltpu.get_barrier_semaphore()
    for j in range(1, GROUP):
        pl.semaphore_signal(barrier, inc=1, device_id=(s, lax.rem(i + j, GROUP)), device_id_type=MESH)
    for peer in (right, left, across):
        pl.semaphore_signal(barrier, inc=1, device_id=peer, device_id_type=MESH)
    for j in range(1, X):
        pl.semaphore_signal(
            barrier, inc=1, device_id=(seq_of(lax.rem(x + j, X), y, z), i), device_id_type=MESH
        )

    for xo in range(1, X):
        @pl.when(xo > x)
        def _():
            for got in gots:
                got[pl.ds(xo * PLANE * 2, PLANE * 2)] = jnp.zeros((PLANE * 2, BLOCK, WIDTH), jnp.bfloat16)

    pl.semaphore_wait(barrier, GROUP - 1 + 3 + X - 1)

    def rows_of(p):
        return pl.ds(pl.multiple_of(p * ROWS, ROWS), ROWS)

    def head_copy(kv, p):
        src, send, recv = ((k_in, k_send, k_recv), (v_in, v_send, v_recv))[kv]
        col = pl.multiple_of(mirrored(z, p) * WIDTH, WIDTH)
        return pltpu.make_async_remote_copy(
            src_ref=src.at[:, :, pl.ds(col, WIDTH)],
            dst_ref=(own_k, own_v)[kv].at[pl.ds(2 * i, 2)],
            send_sem=send.at[p], recv_sem=recv.at[i],
            device_id=(s, p), device_id_type=MESH,
        )

    def head_arrival(kv, p):
        src, send, recv = ((k_in, k_send, k_recv), (v_in, v_send, v_recv))[kv]
        return pltpu.make_async_remote_copy(
            src_ref=src.at[:, :, pl.ds(0, WIDTH)],
            dst_ref=(own_k, own_v)[kv].at[pl.ds(2 * p, 2)],
            send_sem=send.at[p], recv_sem=recv.at[p],
            device_id=(s, p), device_id_type=MESH,
        )

    def q_copy(p):
        col = pl.multiple_of(mirrored(z, p) * QW, WIDTH)
        return pltpu.make_async_remote_copy(
            src_ref=q_in.at[:, pl.ds(col, QW)],
            dst_ref=q_all.at[rows_of(i), :],
            send_sem=q_send.at[p], recv_sem=q_recv.at[i],
            device_id=(s, p), device_id_type=MESH,
        )

    def q_arrival(p):
        return pltpu.make_async_remote_copy(
            src_ref=q_in.at[:, pl.ds(0, QW)],
            dst_ref=q_all.at[rows_of(p), :],
            send_sem=q_send.at[p], recv_sem=q_recv.at[p],
            device_id=(s, p), device_id_type=MESH,
        )

    own_col = pl.multiple_of(h * WIDTH, WIDTH)
    own = [
        pltpu.make_async_copy(k_in.at[:, :, pl.ds(own_col, WIDTH)], own_k.at[pl.ds(2 * i, 2)], local_sem.at[0]),
        pltpu.make_async_copy(v_in.at[:, :, pl.ds(own_col, WIDTH)], own_v.at[pl.ds(2 * i, 2)], local_sem.at[1]),
        pltpu.make_async_copy(
            q_in.at[:, pl.ds(pl.multiple_of(h * QW, WIDTH), QW)], q_all.at[rows_of(i), :], local_sem.at[2]
        ),
    ]
    for kv in range(2):
        for j in (4, 3, 5, 2, 6, 1, 7):
            head_copy(kv, lax.rem(i + j, GROUP)).start()
        own[kv].start()
    for j in (4, 3, 5, 2, 6, 1, 7):
        q_copy(lax.rem(i + j, GROUP)).start()
    own[2].start()

    def item(kv, g, t, other):
        return (items_k, items_v)[kv][other + 2 * place(g, t)]

    def ring_copy(g, t, other, kv):
        return pltpu.make_async_remote_copy(
            src_ref=item(kv, g, t, other), dst_ref=item(kv, g, t + 1, other),
            send_sem=y_send.at[g, t, other, kv], recv_sem=y_recv.at[g, t, other, kv],
            device_id=(right, left)[g], device_id_type=MESH,
        )

    def z_copy(kv):
        return pltpu.make_async_remote_copy(
            src_ref=item(kv, 0, 0, 0), dst_ref=item(kv, 0, 0, 1), send_sem=z_send.at[kv], recv_sem=z_recv.at[kv],
            device_id=across, device_id_type=MESH,
        )

    def x_copy(kv, dx, o):
        return pltpu.make_async_remote_copy(
            src_ref=picks[kv].at[dx - 1, pl.ds(o * 2, 2)],
            dst_ref=gots[kv].at[pl.ds((x * PLANE + o) * 2, 2)],
            send_sem=x_send.at[kv, dx - 1, o], recv_sem=x_recv.at[kv, x, o],
            device_id=(seq_of(lax.rem(x + dx, X), y, z), i), device_id_type=MESH,
        )

    def x_arrival(kv, xo, o):
        return pltpu.make_async_remote_copy(
            src_ref=picks[kv].at[0, pl.ds(o * 2, 2)],
            dst_ref=gots[kv].at[pl.ds((xo * PLANE + o) * 2, 2)],
            send_sem=x_send.at[kv, 0, o], recv_sem=x_recv.at[kv, xo, o],
            device_id=(seq_of(xo, y, z), i), device_id_type=MESH,
        )

    def select(kv, src, o):
        for e in range(2):
            at = fetch[(x * PLANE + o) * 2 + e]
            gots[kv][(x * PLANE + o) * 2 + e] = src[at]
        for dx in range(1, X):
            @pl.when(x + dx < X)
            def _():
                for e in range(2):
                    at = fetch[((x + dx) * PLANE + o) * 2 + e]
                    picks[kv][dx - 1, o * 2 + e] = src[at]

    def forward(kv, o):
        for dx in range(1, X):
            @pl.when(x + dx < X)
            def _():
                x_copy(kv, dx, o).start()

    pending = []

    def pick(kv, g, t, other):
        ay = lax.rem(y + (Y - t if g == 0 else t), Y)
        o = ay * Z + (1 - z if other else z)
        select(kv, item(kv, g, t, other), o)
        pending.append((kv, o))
        if len(pending) > 1:
            forward(*pending.pop(0))

    for kv in range(2):
        own[kv].wait()
        for j in range(1, GROUP):
            head_arrival(kv, lax.rem(i + j, GROUP)).wait_recv()
        ring_copy(0, 0, 0, kv).start()
        ring_copy(1, 0, 0, kv).start()
        z_copy(kv).start()
        pick(kv, 0, 0, 0)
    for kv in range(2):
        z_copy(kv).wait_recv()
        ring_copy(0, 0, 1, kv).start()
        ring_copy(1, 0, 1, kv).start()
        pick(kv, 0, 0, 1)
    half = Y // 2
    for t in range(1, half + 1):
        for other in range(2):
            for kv in range(2):
                for g in range(2):
                    if t == half and kv != g:
                        continue
                    ring_copy(g, t - 1, other, kv).wait_recv()
                    if t < half - 1 or (t == half - 1 and kv == g):
                        ring_copy(g, t, other, kv).start()
                    pick(kv, g, t, other)
    while pending:
        forward(*pending.pop(0))

    own[2].wait()
    for j in range(1, GROUP):
        q_arrival(lax.rem(i + j, GROUP)).wait_recv()
    for xo in range(X - 1):
        @pl.when(xo < x)
        def _():
            def one(o, carry):
                for kv in range(2):
                    x_arrival(kv, xo, o).wait_recv()
                return carry
            lax.fori_loop(0, PLANE, one, 0)

    def out_copy(p, half_block):
        return pltpu.make_async_remote_copy(
            src_ref=out_buf.at[pl.ds(pl.multiple_of((p * 2 + half_block) * BLOCK, BLOCK), BLOCK), :],
            dst_ref=o_out.at[pl.ds(half_block * BLOCK, BLOCK), pl.ds(pl.multiple_of(h * QW, WIDTH), QW)],
            send_sem=o_send.at[p, half_block], recv_sem=o_recv.at[i, half_block],
            device_id=(s, p), device_id_type=MESH,
        )

    def out_arrival(p, half_block):
        return pltpu.make_async_remote_copy(
            src_ref=out_buf.at[pl.ds(half_block * BLOCK, BLOCK), :],
            dst_ref=o_out.at[
                pl.ds(half_block * BLOCK, BLOCK), pl.ds(pl.multiple_of(mirrored(z, p) * QW, WIDTH), QW)
            ],
            send_sem=o_send.at[p, half_block], recv_sem=o_recv.at[p, half_block],
            device_id=(s, p), device_id_type=MESH,
        )

    contract_last = (((1,), (1,)), ((), ()))
    contract = (((1,), (0,)), ((), ()))

    def attend(b):
        first = pl.multiple_of(b * BLOCK, BLOCK)
        q_rows = q_all[pl.ds(first, BLOCK), :]
        q = jnp.concatenate([q_rows[:, g * WIDTH:(g + 1) * WIDTH] for g in range(REPEAT)], axis=0)
        slots = [choose[b, e] for e in range(ENTRIES)]
        k_listed = jnp.concatenate([got_k[slot] for slot in slots], axis=0)
        k_own = own_k[b]
        far = lax.dot_general(q, k_listed, contract_last, preferred_element_type=jnp.float32)
        near = lax.dot_general(q, k_own, contract_last, preferred_element_type=jnp.float32)
        column = lax.broadcasted_iota(jnp.int32, (1, ENTRIES * BLOCK), 1)
        far = jnp.where(column < live[b] * BLOCK, far, -jnp.inf)
        row = lax.rem(lax.broadcasted_iota(jnp.int32, (REPEAT * BLOCK, BLOCK), 0), BLOCK)
        near = jnp.where(lax.broadcasted_iota(jnp.int32, (REPEAT * BLOCK, BLOCK), 1) <= row, near, -jnp.inf)
        highest = jnp.maximum(jnp.max(far, axis=1, keepdims=True), jnp.max(near, axis=1, keepdims=True)) * SCALE
        far = jnp.exp2(far * SCALE - highest)
        near = jnp.exp2(near * SCALE - highest)
        totals = jnp.sum(far, axis=1, keepdims=True) + jnp.sum(near, axis=1, keepdims=True)
        v_listed = jnp.concatenate([got_v[slot] for slot in slots], axis=0)
        v_own = own_v[b]
        mixed = lax.dot_general(far.astype(jnp.bfloat16), v_listed, contract, preferred_element_type=jnp.float32)
        mixed += lax.dot_general(near.astype(jnp.bfloat16), v_own, contract, preferred_element_type=jnp.float32)
        result = (mixed / totals).astype(jnp.bfloat16)
        for g in range(REPEAT):
            out_buf[pl.ds(first, BLOCK), g * WIDTH:(g + 1) * WIDTH] = result[g * BLOCK:(g + 1) * BLOCK]

    def one_pair(t, carry):
        p = xor3(7 - i, t)
        attend(p * 2)

        @pl.when(t > 0)
        def _():
            out_copy(xor3(7 - i, t - 1), 1).start()

        attend(p * 2 + 1)

        @pl.when(t < GROUP - 1)
        def _():
            out_copy(p, 0).start()
        return carry

    lax.fori_loop(0, GROUP, one_pair, 0)
    back = pltpu.make_async_copy(
        out_buf.at[rows_of(i), :], o_out.at[:, pl.ds(pl.multiple_of(h * QW, WIDTH), QW)], local_sem.at[3]
    )
    back.start()

    for j in range(1, GROUP):
        p = lax.rem(i + j, GROUP)
        for kv in range(2):
            head_copy(kv, p).wait_send()
        q_copy(p).wait_send()
        for half_block in range(2):
            out_copy(p, half_block).wait_send()
    for kv in range(2):
        z_copy(kv).wait_send()
    for t in range(half):
        for other in range(2):
            for kv in range(2):
                for g in range(2):
                    if t < half - 1 or kv == g:
                        ring_copy(g, t, other, kv).wait_send()
    for dx in range(1, X):
        @pl.when(x + dx < X)
        def _():
            def one(o, carry):
                for kv in range(2):
                    x_copy(kv, dx, o).wait_send()
                return carry
            lax.fori_loop(0, PLANE, one, 0)
    back.wait()
    for j in range(1, GROUP):
        p = lax.rem(i + j, GROUP)
        for half_block in range(2):
            out_arrival(p, half_block).wait_recv()


def body(queries, keys, values, fetch_list, choose, live):
    s = lax.axis_index("seq")
    fetch = fetch_list.reshape(X, PLANE, X, PLANE, 2)
    fetch = lax.dynamic_index_in_dim(fetch, lax.rem(s, PLANE), 1, keepdims=False)
    fetch = lax.dynamic_index_in_dim(fetch, s // PLANE, 1, keepdims=False).reshape(-1)
    dma = pltpu.SemaphoreType.DMA
    half = Y // 2
    smem = pl.BlockSpec(memory_space=pltpu.SMEM)
    anywhere = pl.BlockSpec(memory_space=pl.ANY)
    bf16 = jnp.bfloat16
    return pl.pallas_call(
        kernel,
        out_shape=jax.ShapeDtypeStruct(queries.shape, bf16),
        in_specs=[smem, smem, smem, anywhere, anywhere, anywhere],
        out_specs=anywhere,
        scratch_shapes=[
            pltpu.VMEM((TOKENS, QW), bf16),
            pltpu.VMEM((TOKENS, QW), bf16),
            [pltpu.VMEM((BLOCKS, BLOCK, WIDTH), bf16)] * PLANE,
            [pltpu.VMEM((BLOCKS, BLOCK, WIDTH), bf16)] * PLANE,
            pltpu.VMEM((X - 1, PLANE * 2, BLOCK, WIDTH), bf16),
            pltpu.VMEM((X - 1, PLANE * 2, BLOCK, WIDTH), bf16),
            pltpu.VMEM((X * PLANE * 2, BLOCK, WIDTH), bf16),
            pltpu.VMEM((X * PLANE * 2, BLOCK, WIDTH), bf16),
            dma((GROUP,)), dma((GROUP,)), dma((GROUP,)), dma((GROUP,)), dma((GROUP,)), dma((GROUP,)),
            dma((2,)), dma((2,)),
            dma((2, half, 2, 2)), dma((2, half, 2, 2)),
            dma((2, X - 1, PLANE)), dma((2, X, PLANE)),
            dma((GROUP, 2)), dma((GROUP, 2)),
            dma((4,)),
        ],
        compiler_params=pltpu.CompilerParams(
            collective_id=0, has_side_effects=True, vmem_limit_bytes=56 * 1024 * 1024
        ),
    )(fetch, choose, live, queries, keys.reshape(-1, BLOCK, keys.shape[1]), values.reshape(-1, BLOCK, values.shape[1]))


def solution(mesh):
    placed = (
        P(("seq", "head"), None),
        P(("seq", "head"), None),
        P(("seq", "head"), None),
        P(),
        P("seq", None),
        P("seq"),
    )
    return jax.shard_map(
        body, mesh=mesh, in_specs=placed, out_specs=P(("seq", "head"), None), check_vma=False
    )
```

```python
import functools
import math

import jax
import jax.numpy as jnp
from jax import lax
from jax.experimental import pallas as pl
from jax.experimental.pallas import tpu as pltpu
from jax.sharding import PartitionSpec as P

MESH = pl.DeviceIdType.MESH
WIDTH = 128
BLOCK = 64
ENTRIES = 16
X, Y, Z = 4, 8, 2
PLANE = Y * Z
GROUP = 8
REPEAT = 5
ROWS = 128
TOKENS = GROUP * ROWS
BLOCKS = TOKENS // BLOCK
QW = REPEAT * WIDTH
LAG = 4
SCALE = math.log2(math.e) / math.sqrt(WIDTH)


def mirrored(z, i):
    return i + z * (6 + 2 * lax.rem(i, 2) - 2 * i)


def xor3(a, b):
    out = 0
    for bit in (4, 2, 1):
        out = out + bit * lax.rem(lax.rem(a // bit, 2) + lax.rem(b // bit, 2), 2)
    return out


def place(g, t):
    return t if g == 0 or t in (0, Y // 2) else Y // 2 + t


def kernel(
    fetch, choose, live, q_in, k_in, v_in, o_out,
    q_all, out_buf, items_k, items_v, pick_k, pick_v, relay_k, relay_v, got_k, got_v,
    q_send, q_recv, k_send, k_recv, v_send, v_recv,
    z_send, z_recv, y_send, y_recv, x_send, x_recv, w_send, w_recv, r_send, r_recv, o_send, o_recv, local_sem,
):
    s = lax.axis_index("seq")
    i = lax.axis_index("head")
    x, y, z = s // PLANE, lax.rem(s // Z, Y), lax.rem(s, Z)
    h = mirrored(z, i)
    own_k, own_v = items_k[0], items_v[0]
    gots = (got_k, got_v)

    def seq_of(ax, ay, az):
        return (ax * Y + ay) * Z + az

    right = (seq_of(x, lax.rem(y + 1, Y), z), i)
    left = (seq_of(x, lax.rem(y + Y - 1, Y), z), i)
    twin = mirrored(1 - z, h)
    across = (seq_of(x, y, 1 - z), twin)

    barrier = pltpu.get_barrier_semaphore()
    for j in range(1, GROUP):
        pl.semaphore_signal(barrier, inc=1, device_id=(s, lax.rem(i + j, GROUP)), device_id_type=MESH)
    for peer in (right, left, across):
        pl.semaphore_signal(barrier, inc=1, device_id=peer, device_id_type=MESH)
    for j in range(1, X):
        for az, ai in ((z, i), (1 - z, twin)):
            pl.semaphore_signal(
                barrier, inc=1, device_id=(seq_of(lax.rem(x + j, X), y, az), ai), device_id_type=MESH
            )

    for xo in range(1, X):
        @pl.when(xo > x)
        def _():
            for got in gots:
                got[pl.ds(xo * PLANE * 2, PLANE * 2)] = jnp.zeros((PLANE * 2, BLOCK, WIDTH), jnp.bfloat16)

    pl.semaphore_wait(barrier, GROUP - 1 + 3 + 2 * (X - 1))

    def rows_of(p):
        return pl.ds(pl.multiple_of(p * ROWS, ROWS), ROWS)

    def head_copy(kv, p):
        src, send, recv = ((k_in, k_send, k_recv), (v_in, v_send, v_recv))[kv]
        col = pl.multiple_of(mirrored(z, p) * WIDTH, WIDTH)
        return pltpu.make_async_remote_copy(
            src_ref=src.at[:, :, pl.ds(col, WIDTH)],
            dst_ref=(own_k, own_v)[kv].at[pl.ds(2 * i, 2)],
            send_sem=send.at[p], recv_sem=recv.at[i],
            device_id=(s, p), device_id_type=MESH,
        )

    def head_arrival(kv, p):
        src, send, recv = ((k_in, k_send, k_recv), (v_in, v_send, v_recv))[kv]
        return pltpu.make_async_remote_copy(
            src_ref=src.at[:, :, pl.ds(0, WIDTH)],
            dst_ref=(own_k, own_v)[kv].at[pl.ds(2 * p, 2)],
            send_sem=send.at[p], recv_sem=recv.at[p],
            device_id=(s, p), device_id_type=MESH,
        )

    def q_copy(p):
        col = pl.multiple_of(mirrored(z, p) * QW, WIDTH)
        return pltpu.make_async_remote_copy(
            src_ref=q_in.at[:, pl.ds(col, QW)],
            dst_ref=q_all.at[rows_of(i), :],
            send_sem=q_send.at[p], recv_sem=q_recv.at[i],
            device_id=(s, p), device_id_type=MESH,
        )

    def q_arrival(p):
        return pltpu.make_async_remote_copy(
            src_ref=q_in.at[:, pl.ds(0, QW)],
            dst_ref=q_all.at[rows_of(p), :],
            send_sem=q_send.at[p], recv_sem=q_recv.at[p],
            device_id=(s, p), device_id_type=MESH,
        )

    own_col = pl.multiple_of(h * WIDTH, WIDTH)
    own = [
        pltpu.make_async_copy(k_in.at[:, :, pl.ds(own_col, WIDTH)], own_k.at[pl.ds(2 * i, 2)], local_sem.at[0]),
        pltpu.make_async_copy(v_in.at[:, :, pl.ds(own_col, WIDTH)], own_v.at[pl.ds(2 * i, 2)], local_sem.at[1]),
        pltpu.make_async_copy(
            q_in.at[:, pl.ds(pl.multiple_of(h * QW, WIDTH), QW)], q_all.at[rows_of(i), :], local_sem.at[2]
        ),
    ]
    for kv in range(2):
        for j in (4, 3, 5, 2, 6, 1, 7):
            head_copy(kv, lax.rem(i + j, GROUP)).start()
        own[kv].start()
    for j in (4, 3, 5, 2, 6, 1, 7):
        q_copy(lax.rem(i + j, GROUP)).start()
    own[2].start()

    def item(kv, g, t, other):
        return items_v[place(g, t)] if kv else items_k[other + 2 * place(g, t)]

    def ring_copy(g, t, other, kv):
        return pltpu.make_async_remote_copy(
            src_ref=item(kv, g, t, other), dst_ref=item(kv, g, t + 1, other),
            send_sem=y_send.at[g, t, other, kv], recv_sem=y_recv.at[g, t, other, kv],
            device_id=(right, left)[g], device_id_type=MESH,
        )

    def z_copy(kv):
        return pltpu.make_async_remote_copy(
            src_ref=item(kv, 0, 0, 0), dst_ref=item(kv, 0, 0, 1), send_sem=z_send.at[kv], recv_sem=z_recv.at[kv],
            device_id=across, device_id_type=MESH,
        )

    def wanted(ax, az, o, e):
        return fetch[((ax * Z + az) * PLANE + o) * 2 + e]

    def x_copy(dx, o):
        return pltpu.make_async_remote_copy(
            src_ref=pick_k.at[dx - 1, pl.ds(o * 2, 2)],
            dst_ref=got_k.at[pl.ds((x * PLANE + o) * 2, 2)],
            send_sem=x_send.at[dx - 1, o], recv_sem=x_recv.at[x, o],
            device_id=(seq_of(lax.rem(x + dx, X), y, z), i), device_id_type=MESH,
        )

    def x_arrival(xo, o):
        return pltpu.make_async_remote_copy(
            src_ref=pick_k.at[0, pl.ds(o * 2, 2)],
            dst_ref=got_k.at[pl.ds((xo * PLANE + o) * 2, 2)],
            send_sem=x_send.at[0, o], recv_sem=x_recv.at[xo, o],
            device_id=(seq_of(xo, y, z), i), device_id_type=MESH,
        )

    def w_copy(dx, dz, oy):
        return pltpu.make_async_remote_copy(
            src_ref=pick_v.at[dx * Z + dz, pl.ds(oy * 2, 2)],
            dst_ref=got_v.at[pl.ds((x * PLANE + oy * Z + z) * 2, 2)],
            send_sem=w_send.at[dx * Z + dz, oy], recv_sem=w_recv.at[x, oy * Z + z],
            device_id=(seq_of(lax.rem(x + dx, X), y, 1 - z if dz else z), twin if dz else i), device_id_type=MESH,
        )

    def w_arrival(xo, o):
        return pltpu.make_async_remote_copy(
            src_ref=pick_v.at[0, pl.ds(0, 2)],
            dst_ref=got_v.at[pl.ds((xo * PLANE + o) * 2, 2)],
            send_sem=w_send.at[0, 0], recv_sem=w_recv.at[xo, o],
            device_id=across, device_id_type=MESH,
        )

    def relay_parts(kv, oy, o):
        if kv == 0:
            yield pick_k.at[1, pl.ds(o * 2, 2)], x_send.at[1, o], relay_k.at[pl.ds(o * 2, 2)], o, (
                got_k.at[pl.ds(o * 2, 2)], x_recv.at[0, o], (seq_of(2, y, z), i))
        else:
            for dz in range(2):
                yield pick_v.at[2 * Z + dz, pl.ds(oy * 2, 2)], w_send.at[2 * Z + dz, oy], relay_v.at[dz, pl.ds(oy * 2, 2)], (
                    PLANE + dz * Y + oy), (
                    got_v.at[pl.ds((oy * Z + z) * 2, 2)], w_recv.at[0, oy * Z + z],
                    (seq_of(2, y, 1 - z if dz else z), twin if dz else i))

    def relay_in(kv, oy, o):
        return [
            pltpu.make_async_remote_copy(
                src_ref=src, dst_ref=buf, send_sem=send, recv_sem=r_recv.at[n],
                device_id=(seq_of(X - 1, y, z), i), device_id_type=MESH,
            )
            for src, send, buf, n, _ in relay_parts(kv, oy, o)
        ]

    def relay_out(kv, oy, o):
        return [
            pltpu.make_async_remote_copy(
                src_ref=buf, dst_ref=to[0], send_sem=r_send.at[n], recv_sem=to[1],
                device_id=to[2], device_id_type=MESH,
            )
            for _, _, buf, n, to in relay_parts(kv, oy, o)
        ]

    def select(kv, src, oy, o):
        for e in range(2):
            gots[kv][(x * PLANE + o) * 2 + e] = src[wanted(x, z, o, e)]
        for dx in range(X):
            @pl.when(x + dx < X)
            def _():
                for e in range(2):
                    if kv == 0 and dx > 0:
                        pick_k[dx - 1, o * 2 + e] = src[wanted(x + dx, z, o, e)]
                    if kv == 1:
                        pick_v[dx * Z + 1, oy * 2 + e] = src[wanted(x + dx, 1 - z, o, e)]
                        if dx > 0:
                            pick_v[dx * Z, oy * 2 + e] = src[wanted(x + dx, z, o, e)]

    def forward(kv, oy, o):
        for dx in range(X - 1, -1, -1):
            def direct():
                if kv == 1:
                    w_copy(dx, 1, oy).start()
                if dx > 0:
                    (x_copy(dx, o) if kv == 0 else w_copy(dx, 0, oy)).start()
            if dx == 2:
                @pl.when(x == 0)
                def _():
                    for copy in relay_in(kv, oy, o):
                        copy.start()
                pl.when(x == 1)(direct)
            else:
                pl.when(x + dx < X)(direct)

    def relay(kv, oy, o):
        @pl.when(x == X - 1)
        def _():
            for copy in relay_in(kv, oy, o):
                copy.wait_recv()
            for copy in relay_out(kv, oy, o):
                copy.start()

    pending = []

    def pick(kv, g, t, other):
        oy = lax.rem(y + (Y - t if g == 0 else t), Y)
        o = oy * Z + (1 - z if other else z)
        select(kv, item(kv, g, t, other), oy, o)
        pending.append((kv, oy, o))
        if len(pending) > 1:
            forward(*pending[-2])
        if len(pending) > LAG:
            relay(*pending[-LAG - 1])

    for kv in range(2):
        own[kv].wait()
        for j in range(1, GROUP):
            head_arrival(kv, lax.rem(i + j, GROUP)).wait_recv()
        ring_copy(0, 0, 0, kv).start()
        ring_copy(1, 0, 0, kv).start()
        if kv == 0:
            z_copy(0).start()
        pick(kv, 0, 0, 0)
    z_copy(0).wait_recv()
    ring_copy(0, 0, 1, 0).start()
    ring_copy(1, 0, 1, 0).start()
    pick(0, 0, 0, 1)
    half = Y // 2
    travels = ((1, 0), (0, 0), (0, 1))
    for t in range(1, half + 1):
        for kv, other in travels:
            for g in range(2):
                if t == half and g != (kv + other) % 2:
                    continue
                ring_copy(g, t - 1, other, kv).wait_recv()
                if t < half - 1 or (t == half - 1 and g == (kv + other) % 2):
                    ring_copy(g, t, other, kv).start()
                pick(kv, g, t, other)
    forward(*pending[-1])
    for step in pending[-LAG:]:
        relay(*step)

    own[2].wait()
    for j in range(1, GROUP):
        q_arrival(lax.rem(i + j, GROUP)).wait_recv()
    for xo in range(X):
        @pl.when(xo < x)
        def _():
            def one(o, carry):
                x_arrival(xo, o).wait_recv()
                w_arrival(xo, o).wait_recv()
                return carry
            lax.fori_loop(0, PLANE, one, 0)
    for oy in range(Y):
        w_arrival(x, oy * Z + 1 - z).wait_recv()

    def out_copy(p, half_block):
        return pltpu.make_async_remote_copy(
            src_ref=out_buf.at[pl.ds(pl.multiple_of((p * 2 + half_block) * BLOCK, BLOCK), BLOCK), :],
            dst_ref=o_out.at[pl.ds(half_block * BLOCK, BLOCK), pl.ds(pl.multiple_of(h * QW, WIDTH), QW)],
            send_sem=o_send.at[p, half_block], recv_sem=o_recv.at[i, half_block],
            device_id=(s, p), device_id_type=MESH,
        )

    def out_arrival(p, half_block):
        return pltpu.make_async_remote_copy(
            src_ref=out_buf.at[pl.ds(half_block * BLOCK, BLOCK), :],
            dst_ref=o_out.at[
                pl.ds(half_block * BLOCK, BLOCK), pl.ds(pl.multiple_of(mirrored(z, p) * QW, WIDTH), QW)
            ],
            send_sem=o_send.at[p, half_block], recv_sem=o_recv.at[p, half_block],
            device_id=(s, p), device_id_type=MESH,
        )

    contract_last = (((1,), (1,)), ((), ()))
    contract = (((1,), (0,)), ((), ()))

    def attend(b):
        first = pl.multiple_of(b * BLOCK, BLOCK)
        q_rows = q_all[pl.ds(first, BLOCK), :]
        q = jnp.concatenate([q_rows[:, g * WIDTH:(g + 1) * WIDTH] for g in range(REPEAT)], axis=0)
        slots = [choose[b, e] for e in range(ENTRIES)]
        k_listed = jnp.concatenate([got_k[slot] for slot in slots], axis=0)
        k_own = own_k[b]
        far = lax.dot_general(q, k_listed, contract_last, preferred_element_type=jnp.float32)
        near = lax.dot_general(q, k_own, contract_last, preferred_element_type=jnp.float32)
        column = lax.broadcasted_iota(jnp.int32, (1, ENTRIES * BLOCK), 1)
        far = jnp.where(column < live[b] * BLOCK, far, -jnp.inf)
        row = lax.rem(lax.broadcasted_iota(jnp.int32, (REPEAT * BLOCK, BLOCK), 0), BLOCK)
        near = jnp.where(lax.broadcasted_iota(jnp.int32, (REPEAT * BLOCK, BLOCK), 1) <= row, near, -jnp.inf)
        highest = jnp.maximum(jnp.max(far, axis=1, keepdims=True), jnp.max(near, axis=1, keepdims=True)) * SCALE
        far = jnp.exp2(far * SCALE - highest)
        near = jnp.exp2(near * SCALE - highest)
        totals = jnp.sum(far, axis=1, keepdims=True) + jnp.sum(near, axis=1, keepdims=True)
        v_listed = jnp.concatenate([got_v[slot] for slot in slots], axis=0)
        v_own = own_v[b]
        mixed = lax.dot_general(far.astype(jnp.bfloat16), v_listed, contract, preferred_element_type=jnp.float32)
        mixed += lax.dot_general(near.astype(jnp.bfloat16), v_own, contract, preferred_element_type=jnp.float32)
        result = (mixed / totals).astype(jnp.bfloat16)
        for g in range(REPEAT):
            out_buf[pl.ds(first, BLOCK), g * WIDTH:(g + 1) * WIDTH] = result[g * BLOCK:(g + 1) * BLOCK]

    def one_pair(t, carry):
        p = xor3(7 - i, t)
        attend(p * 2)

        @pl.when(t > 0)
        def _():
            out_copy(xor3(7 - i, t - 1), 1).start()

        attend(p * 2 + 1)

        @pl.when(t < GROUP - 1)
        def _():
            out_copy(p, 0).start()
        return carry

    lax.fori_loop(0, GROUP, one_pair, 0)
    back = pltpu.make_async_copy(
        out_buf.at[rows_of(i), :], o_out.at[:, pl.ds(pl.multiple_of(h * QW, WIDTH), QW)], local_sem.at[3]
    )
    back.start()

    for j in range(1, GROUP):
        p = lax.rem(i + j, GROUP)
        for kv in range(2):
            head_copy(kv, p).wait_send()
        q_copy(p).wait_send()
        for half_block in range(2):
            out_copy(p, half_block).wait_send()
    z_copy(0).wait_send()
    for t in range(half):
        for kv, other in travels:
            for g in range(2):
                if t < half - 1 or g == (kv + other) % 2:
                    ring_copy(g, t, other, kv).wait_send()
    for dx in range(X):
        @pl.when(x + dx < X)
        def _():
            def one(oy, carry):
                w_copy(dx, 1, oy).wait_send()
                if dx > 0:
                    w_copy(dx, 0, oy).wait_send()
                    x_copy(dx, oy * Z).wait_send()
                    x_copy(dx, oy * Z + 1).wait_send()
                return carry
            lax.fori_loop(0, Y, one, 0)
    @pl.when(x == X - 1)
    def _():
        def one(oy, carry):
            for kv, az in ((0, 0), (0, 1), (1, z)):
                for copy in relay_out(kv, oy, oy * Z + az):
                    copy.wait_send()
            return carry
        lax.fori_loop(0, Y, one, 0)
    back.wait()
    for j in range(1, GROUP):
        p = lax.rem(i + j, GROUP)
        for half_block in range(2):
            out_arrival(p, half_block).wait_recv()


def body(queries, keys, values, fetch_list, choose, live):
    s = lax.axis_index("seq")
    fetch = fetch_list.reshape(X, Y, Z, X, PLANE, 2)
    fetch = lax.dynamic_index_in_dim(fetch, lax.rem(s // Z, Y), 1, keepdims=False)
    fetch = lax.dynamic_index_in_dim(fetch, s // PLANE, 2, keepdims=False).reshape(-1)
    dma = pltpu.SemaphoreType.DMA
    half = Y // 2
    smem = pl.BlockSpec(memory_space=pltpu.SMEM)
    anywhere = pl.BlockSpec(memory_space=pl.ANY)
    bf16 = jnp.bfloat16
    return pl.pallas_call(
        kernel,
        out_shape=jax.ShapeDtypeStruct(queries.shape, bf16),
        in_specs=[smem, smem, smem, anywhere, anywhere, anywhere],
        out_specs=anywhere,
        scratch_shapes=[
            pltpu.VMEM((TOKENS, QW), bf16),
            pltpu.VMEM((TOKENS, QW), bf16),
            [pltpu.VMEM((BLOCKS, BLOCK, WIDTH), bf16)] * PLANE,
            [pltpu.VMEM((BLOCKS, BLOCK, WIDTH), bf16)] * Y,
            pltpu.VMEM((X - 1, PLANE * 2, BLOCK, WIDTH), bf16),
            pltpu.VMEM((X * Z, Y * 2, BLOCK, WIDTH), bf16),
            pltpu.VMEM((PLANE * 2, BLOCK, WIDTH), bf16),
            pltpu.VMEM((Z, Y * 2, BLOCK, WIDTH), bf16),
            pltpu.VMEM((X * PLANE * 2, BLOCK, WIDTH), bf16),
            pltpu.VMEM((X * PLANE * 2, BLOCK, WIDTH), bf16),
            dma((GROUP,)), dma((GROUP,)), dma((GROUP,)), dma((GROUP,)), dma((GROUP,)), dma((GROUP,)),
            dma((1,)), dma((1,)),
            dma((2, half, 2, 2)), dma((2, half, 2, 2)),
            dma((X - 1, PLANE)), dma((X, PLANE)),
            dma((X * Z, Y)), dma((X, PLANE)),
            dma((2 * PLANE,)), dma((2 * PLANE,)),
            dma((GROUP, 2)), dma((GROUP, 2)),
            dma((4,)),
        ],
        compiler_params=pltpu.CompilerParams(
            collective_id=0, has_side_effects=True, vmem_limit_bytes=56 * 1024 * 1024
        ),
    )(fetch, choose, live, queries, keys.reshape(-1, BLOCK, keys.shape[1]), values.reshape(-1, BLOCK, values.shape[1]))


def solution(mesh):
    placed = (
        P(("seq", "head"), None),
        P(("seq", "head"), None),
        P(("seq", "head"), None),
        P(),
        P("seq", None),
        P("seq"),
    )
    return jax.shard_map(
        body, mesh=mesh, in_specs=placed, out_specs=P(("seq", "head"), None), check_vma=False
    )
```

```python
import functools
import math

import jax
import jax.numpy as jnp
from jax import lax
from jax.experimental import pallas as pl
from jax.experimental.pallas import tpu as pltpu
from jax.sharding import PartitionSpec as P

MESH = pl.DeviceIdType.MESH
WIDTH = 128
BLOCK = 64
ENTRIES = 16
X, Y, Z = 4, 8, 2
PLANE = Y * Z
GROUP = 8
REPEAT = 5
ROWS = 128
TOKENS = GROUP * ROWS
BLOCKS = TOKENS // BLOCK
QW = REPEAT * WIDTH
Q_FIRST, Q_EVERY = 3, 2
SCALE = math.log2(math.e) / math.sqrt(WIDTH)


def mirrored(z, i):
    return i + z * (6 + 2 * lax.rem(i, 2) - 2 * i)


def xor3(a, b):
    out = 0
    for bit in (4, 2, 1):
        out = out + bit * lax.rem(lax.rem(a // bit, 2) + lax.rem(b // bit, 2), 2)
    return out


def place(g, t):
    return t if g == 0 or t in (0, Y // 2) else Y // 2 + t


def kernel(
    fetch, choose, live, q_in, k_in, v_in, o_out,
    q_all, out_buf, items_k, items_v, pick_k, pick_v, got_k, got_v,
    q_send, q_recv, k_send, k_recv, v_send, v_recv,
    z_send, z_recv, y_send, y_recv, x_send, x_recv, w_send, w_recv, o_send, o_recv, local_sem,
):
    s = lax.axis_index("seq")
    i = lax.axis_index("head")
    x, y, z = s // PLANE, lax.rem(s // Z, Y), lax.rem(s, Z)
    h = mirrored(z, i)
    own_k, own_v = items_k[0], items_v[0]
    gots = (got_k, got_v)

    def seq_of(ax, ay, az):
        return (ax * Y + ay) * Z + az

    right = (seq_of(x, lax.rem(y + 1, Y), z), i)
    left = (seq_of(x, lax.rem(y + Y - 1, Y), z), i)
    twin = mirrored(1 - z, h)
    across = (seq_of(x, y, 1 - z), twin)

    barrier = pltpu.get_barrier_semaphore()
    for j in range(1, GROUP):
        pl.semaphore_signal(barrier, inc=1, device_id=(s, lax.rem(i + j, GROUP)), device_id_type=MESH)
    for peer in (right, left, across):
        pl.semaphore_signal(barrier, inc=1, device_id=peer, device_id_type=MESH)
    for j in range(1, X):
        for az, ai in ((z, i), (1 - z, twin)):
            pl.semaphore_signal(
                barrier, inc=1, device_id=(seq_of(lax.rem(x + j, X), y, az), ai), device_id_type=MESH
            )

    for xo in range(1, X):
        @pl.when(xo > x)
        def _():
            for got in gots:
                got[pl.ds(xo * PLANE * 2, PLANE * 2)] = jnp.zeros((PLANE * 2, BLOCK, WIDTH), jnp.bfloat16)

    pl.semaphore_wait(barrier, GROUP - 1 + 3 + 2 * (X - 1))

    def rows_of(p):
        return pl.ds(pl.multiple_of(p * ROWS, ROWS), ROWS)

    def head_copy(kv, p):
        src, send, recv = ((k_in, k_send, k_recv), (v_in, v_send, v_recv))[kv]
        col = pl.multiple_of(mirrored(z, p) * WIDTH, WIDTH)
        return pltpu.make_async_remote_copy(
            src_ref=src.at[:, :, pl.ds(col, WIDTH)],
            dst_ref=(own_k, own_v)[kv].at[pl.ds(2 * i, 2)],
            send_sem=send.at[p], recv_sem=recv.at[i],
            device_id=(s, p), device_id_type=MESH,
        )

    def head_arrival(kv, p):
        src, send, recv = ((k_in, k_send, k_recv), (v_in, v_send, v_recv))[kv]
        return pltpu.make_async_remote_copy(
            src_ref=src.at[:, :, pl.ds(0, WIDTH)],
            dst_ref=(own_k, own_v)[kv].at[pl.ds(2 * p, 2)],
            send_sem=send.at[p], recv_sem=recv.at[p],
            device_id=(s, p), device_id_type=MESH,
        )

    def q_copy(p):
        col = pl.multiple_of(mirrored(z, p) * QW, WIDTH)
        return pltpu.make_async_remote_copy(
            src_ref=q_in.at[:, pl.ds(col, QW)],
            dst_ref=q_all.at[rows_of(i), :],
            send_sem=q_send.at[p], recv_sem=q_recv.at[i],
            device_id=(s, p), device_id_type=MESH,
        )

    def q_arrival(p):
        return pltpu.make_async_remote_copy(
            src_ref=q_in.at[:, pl.ds(0, QW)],
            dst_ref=q_all.at[rows_of(p), :],
            send_sem=q_send.at[p], recv_sem=q_recv.at[p],
            device_id=(s, p), device_id_type=MESH,
        )

    own_col = pl.multiple_of(h * WIDTH, WIDTH)
    own = [
        pltpu.make_async_copy(k_in.at[:, :, pl.ds(own_col, WIDTH)], own_k.at[pl.ds(2 * i, 2)], local_sem.at[0]),
        pltpu.make_async_copy(v_in.at[:, :, pl.ds(own_col, WIDTH)], own_v.at[pl.ds(2 * i, 2)], local_sem.at[1]),
        pltpu.make_async_copy(
            q_in.at[:, pl.ds(pl.multiple_of(h * QW, WIDTH), QW)], q_all.at[rows_of(i), :], local_sem.at[2]
        ),
    ]
    for kv in range(2):
        for j in (4, 3, 5, 2, 6, 1, 7):
            head_copy(kv, lax.rem(i + j, GROUP)).start()
        own[kv].start()
    own[2].start()

    def item(kv, g, t, other):
        return items_v[place(g, t)] if kv else items_k[other + 2 * place(g, t)]

    def ring_copy(g, t, other, kv):
        src, dst = item(kv, g, t, other), item(kv, g, t + 1, other)
        if t == Y // 2 - 1:
            part = pl.ds(g * (BLOCKS // 2), BLOCKS // 2)
            src, dst = src.at[part], dst.at[part]
        return pltpu.make_async_remote_copy(
            src_ref=src, dst_ref=dst,
            send_sem=y_send.at[g, t, other, kv], recv_sem=y_recv.at[g, t, other, kv],
            device_id=(right, left)[g], device_id_type=MESH,
        )

    def z_copy(kv):
        return pltpu.make_async_remote_copy(
            src_ref=item(kv, 0, 0, 0), dst_ref=item(kv, 0, 0, 1), send_sem=z_send.at[kv], recv_sem=z_recv.at[kv],
            device_id=across, device_id_type=MESH,
        )

    def wanted(ax, az, o, e):
        return fetch[((ax * Z + az) * PLANE + o) * 2 + e]

    def x_copy(dx, o):
        return pltpu.make_async_remote_copy(
            src_ref=pick_k.at[dx - 1, pl.ds(o * 2, 2)],
            dst_ref=got_k.at[pl.ds((x * PLANE + o) * 2, 2)],
            send_sem=x_send.at[dx - 1, o], recv_sem=x_recv.at[x, o],
            device_id=(seq_of(lax.rem(x + dx, X), y, z), i), device_id_type=MESH,
        )

    def x_arrival(xo, o):
        return pltpu.make_async_remote_copy(
            src_ref=pick_k.at[0, pl.ds(o * 2, 2)],
            dst_ref=got_k.at[pl.ds((xo * PLANE + o) * 2, 2)],
            send_sem=x_send.at[0, o], recv_sem=x_recv.at[xo, o],
            device_id=(seq_of(xo, y, z), i), device_id_type=MESH,
        )

    def w_copy(dx, dz, oy):
        return pltpu.make_async_remote_copy(
            src_ref=pick_v.at[dx * Z + dz, pl.ds(oy * 2, 2)],
            dst_ref=got_v.at[pl.ds((x * PLANE + oy * Z + z) * 2, 2)],
            send_sem=w_send.at[dx * Z + dz, oy], recv_sem=w_recv.at[x, oy * Z + z],
            device_id=(seq_of(lax.rem(x + dx, X), y, 1 - z if dz else z), twin if dz else i), device_id_type=MESH,
        )

    def w_arrival(xo, o):
        return pltpu.make_async_remote_copy(
            src_ref=pick_v.at[0, pl.ds(0, 2)],
            dst_ref=got_v.at[pl.ds((xo * PLANE + o) * 2, 2)],
            send_sem=w_send.at[0, 0], recv_sem=w_recv.at[xo, o],
            device_id=across, device_id_type=MESH,
        )

    def select(kv, src, oy, o):
        for e in range(2):
            gots[kv][(x * PLANE + o) * 2 + e] = src[wanted(x, z, o, e)]
        for dx in range(X):
            @pl.when(x + dx < X)
            def _():
                for e in range(2):
                    if kv == 0 and dx > 0:
                        pick_k[dx - 1, o * 2 + e] = src[wanted(x + dx, z, o, e)]
                    if kv == 1:
                        pick_v[dx * Z + 1, oy * 2 + e] = src[wanted(x + dx, 1 - z, o, e)]
                        if dx > 0:
                            pick_v[dx * Z, oy * 2 + e] = src[wanted(x + dx, z, o, e)]

    def forward(kv, oy, o):
        for dx in range(X - 1, -1, -1):
            @pl.when(x + dx < X)
            def _():
                if kv == 1:
                    w_copy(dx, 1, oy).start()
                if dx > 0:
                    (x_copy(dx, o) if kv == 0 else w_copy(dx, 0, oy)).start()

    pending = []
    q_order = [4, 3, 5, 2, 6, 1, 7]

    def pick(kv, g, t, other):
        oy = lax.rem(y + (Y - t if g == 0 else t), Y)
        o = oy * Z + (1 - z if other else z)
        select(kv, item(kv, g, t, other), oy, o)
        pending.append((kv, oy, o))
        if len(pending) > 1:
            forward(*pending[-2])
        if len(pending) >= Q_FIRST and (len(pending) - Q_FIRST) % Q_EVERY == 0 and q_order:
            q_copy(lax.rem(i + q_order.pop(0), GROUP)).start()

    for kv in range(2):
        own[kv].wait()
        for j in range(1, GROUP):
            head_arrival(kv, lax.rem(i + j, GROUP)).wait_recv()
        ring_copy(0, 0, 0, kv).start()
        ring_copy(1, 0, 0, kv).start()
        if kv == 0:
            z_copy(0).start()
        pick(kv, 0, 0, 0)
    z_copy(0).wait_recv()
    ring_copy(0, 0, 1, 0).start()
    ring_copy(1, 0, 1, 0).start()
    pick(0, 0, 0, 1)
    half = Y // 2
    travels = ((1, 0), (0, 0), (0, 1))
    for t in range(1, half + 1):
        for kv, other in travels:
            for g in range(2):
                ring_copy(g, t - 1, other, kv).wait_recv()
                if t < half:
                    ring_copy(g, t, other, kv).start()
                    pick(kv, g, t, other)
            if t == half:
                pick(kv, 0, t, other)
    forward(*pending[-1])
    for j in q_order:
        q_copy(lax.rem(i + j, GROUP)).start()

    own[2].wait()
    for j in range(1, GROUP):
        q_arrival(lax.rem(i + j, GROUP)).wait_recv()
    for xo in range(X):
        @pl.when(xo < x)
        def _():
            def one(o, carry):
                x_arrival(xo, o).wait_recv()
                w_arrival(xo, o).wait_recv()
                return carry
            lax.fori_loop(0, PLANE, one, 0)
    for oy in range(Y):
        w_arrival(x, oy * Z + 1 - z).wait_recv()

    def out_copy(p, half_block):
        return pltpu.make_async_remote_copy(
            src_ref=out_buf.at[pl.ds(pl.multiple_of((p * 2 + half_block) * BLOCK, BLOCK), BLOCK), :],
            dst_ref=o_out.at[pl.ds(half_block * BLOCK, BLOCK), pl.ds(pl.multiple_of(h * QW, WIDTH), QW)],
            send_sem=o_send.at[p, half_block], recv_sem=o_recv.at[i, half_block],
            device_id=(s, p), device_id_type=MESH,
        )

    def out_arrival(p, half_block):
        return pltpu.make_async_remote_copy(
            src_ref=out_buf.at[pl.ds(half_block * BLOCK, BLOCK), :],
            dst_ref=o_out.at[
                pl.ds(half_block * BLOCK, BLOCK), pl.ds(pl.multiple_of(mirrored(z, p) * QW, WIDTH), QW)
            ],
            send_sem=o_send.at[p, half_block], recv_sem=o_recv.at[p, half_block],
            device_id=(s, p), device_id_type=MESH,
        )

    contract_last = (((1,), (1,)), ((), ()))
    contract = (((1,), (0,)), ((), ()))

    def attend(b):
        first = pl.multiple_of(b * BLOCK, BLOCK)
        q_rows = q_all[pl.ds(first, BLOCK), :]
        q = jnp.concatenate([q_rows[:, g * WIDTH:(g + 1) * WIDTH] for g in range(REPEAT)], axis=0)
        slots = [choose[b, e] for e in range(ENTRIES)]
        k_listed = jnp.concatenate([got_k[slot] for slot in slots], axis=0)
        k_own = own_k[b]
        far = lax.dot_general(q, k_listed, contract_last, preferred_element_type=jnp.float32)
        near = lax.dot_general(q, k_own, contract_last, preferred_element_type=jnp.float32)
        column = lax.broadcasted_iota(jnp.int32, (1, ENTRIES * BLOCK), 1)
        far = jnp.where(column < live[b] * BLOCK, far, -jnp.inf)
        row = lax.rem(lax.broadcasted_iota(jnp.int32, (REPEAT * BLOCK, BLOCK), 0), BLOCK)
        near = jnp.where(lax.broadcasted_iota(jnp.int32, (REPEAT * BLOCK, BLOCK), 1) <= row, near, -jnp.inf)
        highest = jnp.maximum(jnp.max(far, axis=1, keepdims=True), jnp.max(near, axis=1, keepdims=True)) * SCALE
        far = jnp.exp2(far * SCALE - highest)
        near = jnp.exp2(near * SCALE - highest)
        totals = jnp.sum(far, axis=1, keepdims=True) + jnp.sum(near, axis=1, keepdims=True)
        v_listed = jnp.concatenate([got_v[slot] for slot in slots], axis=0)
        v_own = own_v[b]
        mixed = lax.dot_general(far.astype(jnp.bfloat16), v_listed, contract, preferred_element_type=jnp.float32)
        mixed += lax.dot_general(near.astype(jnp.bfloat16), v_own, contract, preferred_element_type=jnp.float32)
        result = (mixed / totals).astype(jnp.bfloat16)
        for g in range(REPEAT):
            out_buf[pl.ds(first, BLOCK), g * WIDTH:(g + 1) * WIDTH] = result[g * BLOCK:(g + 1) * BLOCK]

    def one_pair(t, carry):
        p = xor3(7 - i, t)
        attend(p * 2)

        @pl.when(t > 0)
        def _():
            out_copy(xor3(7 - i, t - 1), 1).start()

        attend(p * 2 + 1)

        @pl.when(t < GROUP - 1)
        def _():
            out_copy(p, 0).start()
        return carry

    lax.fori_loop(0, GROUP, one_pair, 0)
    back = pltpu.make_async_copy(
        out_buf.at[rows_of(i), :], o_out.at[:, pl.ds(pl.multiple_of(h * QW, WIDTH), QW)], local_sem.at[3]
    )
    back.start()

    for j in range(1, GROUP):
        p = lax.rem(i + j, GROUP)
        for kv in range(2):
            head_copy(kv, p).wait_send()
        q_copy(p).wait_send()
        for half_block in range(2):
            out_copy(p, half_block).wait_send()
    z_copy(0).wait_send()
    for t in range(half):
        for kv, other in travels:
            for g in range(2):
                ring_copy(g, t, other, kv).wait_send()
    for dx in range(X):
        @pl.when(x + dx < X)
        def _():
            def one(oy, carry):
                w_copy(dx, 1, oy).wait_send()
                if dx > 0:
                    w_copy(dx, 0, oy).wait_send()
                    x_copy(dx, oy * Z).wait_send()
                    x_copy(dx, oy * Z + 1).wait_send()
                return carry
            lax.fori_loop(0, Y, one, 0)
    back.wait()
    for j in range(1, GROUP):
        p = lax.rem(i + j, GROUP)
        for half_block in range(2):
            out_arrival(p, half_block).wait_recv()


def body(queries, keys, values, fetch_list, choose, live):
    s = lax.axis_index("seq")
    fetch = fetch_list.reshape(X, Y, Z, X, PLANE, 2)
    fetch = lax.dynamic_index_in_dim(fetch, lax.rem(s // Z, Y), 1, keepdims=False)
    fetch = lax.dynamic_index_in_dim(fetch, s // PLANE, 2, keepdims=False).reshape(-1)
    dma = pltpu.SemaphoreType.DMA
    half = Y // 2
    smem = pl.BlockSpec(memory_space=pltpu.SMEM)
    anywhere = pl.BlockSpec(memory_space=pl.ANY)
    bf16 = jnp.bfloat16
    return pl.pallas_call(
        kernel,
        out_shape=jax.ShapeDtypeStruct(queries.shape, bf16),
        in_specs=[smem, smem, smem, anywhere, anywhere, anywhere],
        out_specs=anywhere,
        scratch_shapes=[
            pltpu.VMEM((TOKENS, QW), bf16),
            pltpu.VMEM((TOKENS, QW), bf16),
            [pltpu.VMEM((BLOCKS, BLOCK, WIDTH), bf16)] * PLANE,
            [pltpu.VMEM((BLOCKS, BLOCK, WIDTH), bf16)] * Y,
            pltpu.VMEM((X - 1, PLANE * 2, BLOCK, WIDTH), bf16),
            pltpu.VMEM((X * Z, Y * 2, BLOCK, WIDTH), bf16),
            pltpu.VMEM((X * PLANE * 2, BLOCK, WIDTH), bf16),
            pltpu.VMEM((X * PLANE * 2, BLOCK, WIDTH), bf16),
            dma((GROUP,)), dma((GROUP,)), dma((GROUP,)), dma((GROUP,)), dma((GROUP,)), dma((GROUP,)),
            dma((1,)), dma((1,)),
            dma((2, half, 2, 2)), dma((2, half, 2, 2)),
            dma((X - 1, PLANE)), dma((X, PLANE)),
            dma((X * Z, Y)), dma((X, PLANE)),
            dma((GROUP, 2)), dma((GROUP, 2)),
            dma((4,)),
        ],
        compiler_params=pltpu.CompilerParams(
            collective_id=0, has_side_effects=True, vmem_limit_bytes=56 * 1024 * 1024
        ),
    )(fetch, choose, live, queries, keys.reshape(-1, BLOCK, keys.shape[1]), values.reshape(-1, BLOCK, values.shape[1]))


def solution(mesh):
    placed = (
        P(("seq", "head"), None),
        P(("seq", "head"), None),
        P(("seq", "head"), None),
        P(),
        P("seq", None),
        P("seq"),
    )
    return jax.shard_map(
        body, mesh=mesh, in_specs=placed, out_specs=P(("seq", "head"), None), check_vma=False
    )
```

```python
import functools
import math

import jax
import jax.numpy as jnp
from jax import lax
from jax.experimental import pallas as pl
from jax.experimental.pallas import tpu as pltpu
from jax.sharding import PartitionSpec as P

MESH = pl.DeviceIdType.MESH
WIDTH = 128
BLOCK = 64
ENTRIES = 16
X, Y, Z = 4, 8, 2
PLANE = Y * Z
GROUP = 8
REPEAT = 5
ROWS = 128
TOKENS = GROUP * ROWS
BLOCKS = TOKENS // BLOCK
QW = REPEAT * WIDTH
Q_FIRST, Q_EVERY = 3, 2
PIECES = GROUP // 2
SCALE = math.log2(math.e) / math.sqrt(WIDTH)


def mirrored(z, i):
    return i + z * (6 + 2 * lax.rem(i, 2) - 2 * i)


def xor3(a, b):
    out = 0
    for bit in (4, 2, 1):
        out = out + bit * lax.rem(lax.rem(a // bit, 2) + lax.rem(b // bit, 2), 2)
    return out


def place(g, t):
    return t if g == 0 or t in (0, Y // 2) else Y // 2 + t


def xor2(a, n):
    return 2 * lax.rem(a // 2 + n // 2, 2) + lax.rem(lax.rem(a, 2) + n % 2, 2)


def kernel(
    fetch_in, choose, live, q_in, k_in, v_in, o_out,
    fetch, q_all, out_buf, items_k, items_v, pick_k, pick_v, got_k, got_v,
    q_send, q_recv, k_send, k_recv, v_send, v_recv,
    z_send, z_recv, f_send, f_recv, y_send, y_recv, x_send, x_recv, w_send, w_recv, o_send, o_recv, local_sem, f_sem,
):
    s = lax.axis_index("seq")
    i = lax.axis_index("head")
    x, y, z = s // PLANE, lax.rem(s // Z, Y), lax.rem(s, Z)
    h = mirrored(z, i)
    own_k, own_v = items_k[0], items_v[0]
    gots = (got_k, got_v)

    def seq_of(ax, ay, az):
        return (ax * Y + ay) * Z + az

    right = (seq_of(x, lax.rem(y + 1, Y), z), i)
    left = (seq_of(x, lax.rem(y + Y - 1, Y), z), i)
    twin = mirrored(1 - z, h)
    across = (seq_of(x, y, 1 - z), twin)

    barrier = pltpu.get_barrier_semaphore()
    for j in range(1, GROUP):
        pl.semaphore_signal(barrier, inc=1, device_id=(s, lax.rem(i + j, GROUP)), device_id_type=MESH)
    for peer in (right, left, across):
        pl.semaphore_signal(barrier, inc=1, device_id=peer, device_id_type=MESH)
    for j in range(1, X):
        for az, ai in ((z, i), (1 - z, twin)):
            pl.semaphore_signal(
                barrier, inc=1, device_id=(seq_of(lax.rem(x + j, X), y, az), ai), device_id_type=MESH
            )

    fetches = [
        pltpu.make_async_copy(fetch_in.at[seq_of(ax, y, az)], fetch.at[ax * Z + az], f_sem.at[ax * Z + az])
        for ax in range(X) for az in range(Z)
    ]
    for copy in fetches:
        copy.start()

    for xo in range(1, X):
        @pl.when(xo > x)
        def _():
            for got in gots:
                got[pl.ds(xo * PLANE * 2, PLANE * 2)] = jnp.zeros((PLANE * 2, BLOCK, WIDTH), jnp.bfloat16)

    for copy in fetches:
        copy.wait()
    pl.semaphore_wait(barrier, GROUP - 1 + 3 + 2 * (X - 1))

    def rows_of(p):
        return pl.ds(pl.multiple_of(p * ROWS, ROWS), ROWS)

    def head_copy(kv, p):
        src, send, recv = ((k_in, k_send, k_recv), (v_in, v_send, v_recv))[kv]
        col = pl.multiple_of(mirrored(z, p) * WIDTH, WIDTH)
        return pltpu.make_async_remote_copy(
            src_ref=src.at[:, :, pl.ds(col, WIDTH)],
            dst_ref=(own_k, own_v)[kv].at[pl.ds(2 * i, 2)],
            send_sem=send.at[p], recv_sem=recv.at[i],
            device_id=(s, p), device_id_type=MESH,
        )

    def head_arrival(kv, p):
        src, send, recv = ((k_in, k_send, k_recv), (v_in, v_send, v_recv))[kv]
        return pltpu.make_async_remote_copy(
            src_ref=src.at[:, :, pl.ds(0, WIDTH)],
            dst_ref=(own_k, own_v)[kv].at[pl.ds(2 * p, 2)],
            send_sem=send.at[p], recv_sem=recv.at[p],
            device_id=(s, p), device_id_type=MESH,
        )

    def q_copy(p):
        col = pl.multiple_of(mirrored(z, p) * QW, WIDTH)
        return pltpu.make_async_remote_copy(
            src_ref=q_in.at[:, pl.ds(col, QW)],
            dst_ref=q_all.at[rows_of(i), :],
            send_sem=q_send.at[p], recv_sem=q_recv.at[i],
            device_id=(s, p), device_id_type=MESH,
        )

    def q_arrival(p):
        return pltpu.make_async_remote_copy(
            src_ref=q_in.at[:, pl.ds(0, QW)],
            dst_ref=q_all.at[rows_of(p), :],
            send_sem=q_send.at[p], recv_sem=q_recv.at[p],
            device_id=(s, p), device_id_type=MESH,
        )

    own_col = pl.multiple_of(h * WIDTH, WIDTH)
    own = [
        pltpu.make_async_copy(k_in.at[:, :, pl.ds(own_col, WIDTH)], own_k.at[pl.ds(2 * i, 2)], local_sem.at[0]),
        pltpu.make_async_copy(v_in.at[:, :, pl.ds(own_col, WIDTH)], own_v.at[pl.ds(2 * i, 2)], local_sem.at[1]),
        pltpu.make_async_copy(
            q_in.at[:, pl.ds(pl.multiple_of(h * QW, WIDTH), QW)], q_all.at[rows_of(i), :], local_sem.at[2]
        ),
    ]
    for kv in range(2):
        for j in (4, 3, 5, 2, 6, 1, 7):
            head_copy(kv, lax.rem(i + j, GROUP)).start()
        own[kv].start()
    own[2].start()

    def item(kv, g, t, other):
        return items_v[place(g, t)] if kv else items_k[other + 2 * place(g, t)]

    def ring_copy(g, t, other, kv):
        src, dst = item(kv, g, t, other), item(kv, g, t + 1, other)
        if t == Y // 2 - 1:
            part = pl.ds(g * (BLOCKS // 2), BLOCKS // 2)
            src, dst = src.at[part], dst.at[part]
        return pltpu.make_async_remote_copy(
            src_ref=src, dst_ref=dst,
            send_sem=y_send.at[g, t, other, kv], recv_sem=y_recv.at[g, t, other, kv],
            device_id=(right, left)[g], device_id_type=MESH,
        )

    def piece(n):
        return xor2(i // 2, n)

    def first_copy(g, kv, c):
        part = pl.ds(4 * c, 4)
        return pltpu.make_async_remote_copy(
            src_ref=item(kv, g, 0, 0).at[part], dst_ref=item(kv, g, 1, 0).at[part],
            send_sem=f_send.at[g, kv, c], recv_sem=f_recv.at[g, kv, c],
            device_id=(right, left)[g], device_id_type=MESH,
        )

    def ring_wait(g, t, other, kv):
        if t == 0 and other == 0:
            for c in range(PIECES):
                first_copy(g, kv, c).wait_recv()
        else:
            ring_copy(g, t, other, kv).wait_recv()

    def z_copy(kv):
        return pltpu.make_async_remote_copy(
            src_ref=item(kv, 0, 0, 0), dst_ref=item(kv, 0, 0, 1), send_sem=z_send.at[kv], recv_sem=z_recv.at[kv],
            device_id=across, device_id_type=MESH,
        )

    def wanted(ax, az, o, e):
        return fetch[ax * Z + az, e, x * PLANE + o]

    def x_copy(dx, o):
        return pltpu.make_async_remote_copy(
            src_ref=pick_k.at[dx - 1, pl.ds(o * 2, 2)],
            dst_ref=got_k.at[pl.ds((x * PLANE + o) * 2, 2)],
            send_sem=x_send.at[dx - 1, o], recv_sem=x_recv.at[x, o],
            device_id=(seq_of(lax.rem(x + dx, X), y, z), i), device_id_type=MESH,
        )

    def x_arrival(xo, o):
        return pltpu.make_async_remote_copy(
            src_ref=pick_k.at[0, pl.ds(o * 2, 2)],
            dst_ref=got_k.at[pl.ds((xo * PLANE + o) * 2, 2)],
            send_sem=x_send.at[0, o], recv_sem=x_recv.at[xo, o],
            device_id=(seq_of(xo, y, z), i), device_id_type=MESH,
        )

    def w_copy(dx, dz, oy):
        return pltpu.make_async_remote_copy(
            src_ref=pick_v.at[dx * Z + dz, pl.ds(oy * 2, 2)],
            dst_ref=got_v.at[pl.ds((x * PLANE + oy * Z + z) * 2, 2)],
            send_sem=w_send.at[dx * Z + dz, oy], recv_sem=w_recv.at[x, oy * Z + z],
            device_id=(seq_of(lax.rem(x + dx, X), y, 1 - z if dz else z), twin if dz else i), device_id_type=MESH,
        )

    def w_arrival(xo, o):
        return pltpu.make_async_remote_copy(
            src_ref=pick_v.at[0, pl.ds(0, 2)],
            dst_ref=got_v.at[pl.ds((xo * PLANE + o) * 2, 2)],
            send_sem=w_send.at[0, 0], recv_sem=w_recv.at[xo, o],
            device_id=across, device_id_type=MESH,
        )

    def select(kv, src, oy, o):
        for e in range(2):
            gots[kv][(x * PLANE + o) * 2 + e] = src[wanted(x, z, o, e)]
        for dx in range(X):
            @pl.when(x + dx < X)
            def _():
                for e in range(2):
                    if kv == 0 and dx > 0:
                        pick_k[dx - 1, o * 2 + e] = src[wanted(x + dx, z, o, e)]
                    if kv == 1:
                        pick_v[dx * Z + 1, oy * 2 + e] = src[wanted(x + dx, 1 - z, o, e)]
                        if dx > 0:
                            pick_v[dx * Z, oy * 2 + e] = src[wanted(x + dx, z, o, e)]

    def forward(kv, oy, o):
        for dx in range(X - 1, -1, -1):
            @pl.when(x + dx < X)
            def _():
                if kv == 1:
                    w_copy(dx, 1, oy).start()
                if dx > 0:
                    (x_copy(dx, o) if kv == 0 else w_copy(dx, 0, oy)).start()

    pending = []
    q_order = [4, 3, 5, 2, 6, 1, 7]

    def pick(kv, g, t, other):
        oy = lax.rem(y + (Y - t if g == 0 else t), Y)
        o = oy * Z + (1 - z if other else z)
        select(kv, item(kv, g, t, other), oy, o)
        pending.append((kv, oy, o))
        if len(pending) > 1:
            forward(*pending[-2])
        if len(pending) >= Q_FIRST and (len(pending) - Q_FIRST) % Q_EVERY == 0 and q_order:
            q_copy(lax.rem(i + q_order.pop(0), GROUP)).start()

    for kv in range(2):
        own[kv].wait()
        for n in range(PIECES):
            c = piece(n)
            for core in range(2):
                p = 2 * c + core
                if n > 0:
                    head_arrival(kv, p).wait_recv()
                else:
                    @pl.when(p != i)
                    def _():
                        head_arrival(kv, p).wait_recv()
            first_copy(0, kv, c).start()
            first_copy(1, kv, c).start()
        if kv == 0:
            z_copy(0).start()
        pick(kv, 0, 0, 0)
    z_copy(0).wait_recv()
    ring_copy(0, 0, 1, 0).start()
    ring_copy(1, 0, 1, 0).start()
    pick(0, 0, 0, 1)
    half = Y // 2
    travels = ((0, 0), (1, 0), (0, 1))
    for t in range(1, half + 1):
        for kv, other in travels:
            for g in range(2):
                ring_wait(g, t - 1, other, kv)
                if t < half:
                    ring_copy(g, t, other, kv).start()
                    pick(kv, g, t, other)
            if t == half:
                pick(kv, 0, t, other)
    forward(*pending[-1])
    for j in q_order:
        q_copy(lax.rem(i + j, GROUP)).start()

    own[2].wait()
    for j in range(1, GROUP):
        q_arrival(lax.rem(i + j, GROUP)).wait_recv()
    for xo in range(X):
        @pl.when(xo < x)
        def _():
            def one(o, carry):
                x_arrival(xo, o).wait_recv()
                w_arrival(xo, o).wait_recv()
                return carry
            lax.fori_loop(0, PLANE, one, 0)
    for oy in range(Y):
        w_arrival(x, oy * Z + 1 - z).wait_recv()

    def out_copy(p, half_block):
        return pltpu.make_async_remote_copy(
            src_ref=out_buf.at[pl.ds(pl.multiple_of((p * 2 + half_block) * BLOCK, BLOCK), BLOCK), :],
            dst_ref=o_out.at[pl.ds(half_block * BLOCK, BLOCK), pl.ds(pl.multiple_of(h * QW, WIDTH), QW)],
            send_sem=o_send.at[p, half_block], recv_sem=o_recv.at[i, half_block],
            device_id=(s, p), device_id_type=MESH,
        )

    def out_arrival(p, half_block):
        return pltpu.make_async_remote_copy(
            src_ref=out_buf.at[pl.ds(half_block * BLOCK, BLOCK), :],
            dst_ref=o_out.at[
                pl.ds(half_block * BLOCK, BLOCK), pl.ds(pl.multiple_of(mirrored(z, p) * QW, WIDTH), QW)
            ],
            send_sem=o_send.at[p, half_block], recv_sem=o_recv.at[p, half_block],
            device_id=(s, p), device_id_type=MESH,
        )

    contract_last = (((1,), (1,)), ((), ()))
    contract = (((1,), (0,)), ((), ()))

    def attend(b):
        first = pl.multiple_of(b * BLOCK, BLOCK)
        q_rows = q_all[pl.ds(first, BLOCK), :]
        q = jnp.concatenate([q_rows[:, g * WIDTH:(g + 1) * WIDTH] for g in range(REPEAT)], axis=0)
        slots = [choose[b, e] for e in range(ENTRIES)]
        k_listed = jnp.concatenate([got_k[slot] for slot in slots], axis=0)
        k_own = own_k[b]
        far = lax.dot_general(q, k_listed, contract_last, preferred_element_type=jnp.float32)
        near = lax.dot_general(q, k_own, contract_last, preferred_element_type=jnp.float32)
        column = lax.broadcasted_iota(jnp.int32, (1, ENTRIES * BLOCK), 1)
        far = jnp.where(column < live[b] * BLOCK, far, -jnp.inf)
        row = lax.rem(lax.broadcasted_iota(jnp.int32, (REPEAT * BLOCK, BLOCK), 0), BLOCK)
        near = jnp.where(lax.broadcasted_iota(jnp.int32, (REPEAT * BLOCK, BLOCK), 1) <= row, near, -jnp.inf)
        highest = jnp.maximum(jnp.max(far, axis=1, keepdims=True), jnp.max(near, axis=1, keepdims=True)) * SCALE
        far = jnp.exp2(far * SCALE - highest)
        near = jnp.exp2(near * SCALE - highest)
        totals = jnp.sum(far, axis=1, keepdims=True) + jnp.sum(near, axis=1, keepdims=True)
        v_listed = jnp.concatenate([got_v[slot] for slot in slots], axis=0)
        v_own = own_v[b]
        mixed = lax.dot_general(far.astype(jnp.bfloat16), v_listed, contract, preferred_element_type=jnp.float32)
        mixed += lax.dot_general(near.astype(jnp.bfloat16), v_own, contract, preferred_element_type=jnp.float32)
        result = (mixed / totals).astype(jnp.bfloat16)
        for g in range(REPEAT):
            out_buf[pl.ds(first, BLOCK), g * WIDTH:(g + 1) * WIDTH] = result[g * BLOCK:(g + 1) * BLOCK]

    def one_pair(t, carry):
        p = xor3(7 - i, t)
        attend(p * 2)

        @pl.when(t > 0)
        def _():
            out_copy(xor3(7 - i, t - 1), 1).start()

        attend(p * 2 + 1)

        @pl.when(t < GROUP - 1)
        def _():
            out_copy(p, 0).start()
        return carry

    lax.fori_loop(0, GROUP, one_pair, 0)
    back = pltpu.make_async_copy(
        out_buf.at[rows_of(i), :], o_out.at[:, pl.ds(pl.multiple_of(h * QW, WIDTH), QW)], local_sem.at[3]
    )
    back.start()

    for j in range(1, GROUP):
        p = lax.rem(i + j, GROUP)
        for kv in range(2):
            head_copy(kv, p).wait_send()
        q_copy(p).wait_send()
        for half_block in range(2):
            out_copy(p, half_block).wait_send()
    z_copy(0).wait_send()
    for t in range(half):
        for kv, other in travels:
            for g in range(2):
                if t == 0 and other == 0:
                    for c in range(PIECES):
                        first_copy(g, kv, c).wait_send()
                else:
                    ring_copy(g, t, other, kv).wait_send()
    for dx in range(X):
        @pl.when(x + dx < X)
        def _():
            def one(oy, carry):
                w_copy(dx, 1, oy).wait_send()
                if dx > 0:
                    w_copy(dx, 0, oy).wait_send()
                    x_copy(dx, oy * Z).wait_send()
                    x_copy(dx, oy * Z + 1).wait_send()
                return carry
            lax.fori_loop(0, Y, one, 0)
    back.wait()
    for j in range(1, GROUP):
        p = lax.rem(i + j, GROUP)
        for half_block in range(2):
            out_arrival(p, half_block).wait_recv()


def body(queries, keys, values, fetch_list, choose, live):
    fetch = fetch_list.transpose(0, 2, 1)
    dma = pltpu.SemaphoreType.DMA
    half = Y // 2
    smem = pl.BlockSpec(memory_space=pltpu.SMEM)
    anywhere = pl.BlockSpec(memory_space=pl.ANY)
    bf16 = jnp.bfloat16
    return pl.pallas_call(
        kernel,
        out_shape=jax.ShapeDtypeStruct(queries.shape, bf16),
        in_specs=[anywhere, smem, smem, anywhere, anywhere, anywhere],
        out_specs=anywhere,
        scratch_shapes=[
            pltpu.SMEM((X * Z, 2, X * PLANE), jnp.int32),
            pltpu.VMEM((TOKENS, QW), bf16),
            pltpu.VMEM((TOKENS, QW), bf16),
            [pltpu.VMEM((BLOCKS, BLOCK, WIDTH), bf16)] * PLANE,
            [pltpu.VMEM((BLOCKS, BLOCK, WIDTH), bf16)] * Y,
            pltpu.VMEM((X - 1, PLANE * 2, BLOCK, WIDTH), bf16),
            pltpu.VMEM((X * Z, Y * 2, BLOCK, WIDTH), bf16),
            pltpu.VMEM((X * PLANE * 2, BLOCK, WIDTH), bf16),
            pltpu.VMEM((X * PLANE * 2, BLOCK, WIDTH), bf16),
            dma((GROUP,)), dma((GROUP,)), dma((GROUP,)), dma((GROUP,)), dma((GROUP,)), dma((GROUP,)),
            dma((1,)), dma((1,)),
            dma((2, 2, PIECES)), dma((2, 2, PIECES)),
            dma((2, half, 2, 2)), dma((2, half, 2, 2)),
            dma((X - 1, PLANE)), dma((X, PLANE)),
            dma((X * Z, Y)), dma((X, PLANE)),
            dma((GROUP, 2)), dma((GROUP, 2)),
            dma((4,)), dma((X * Z,)),
        ],
        compiler_params=pltpu.CompilerParams(
            collective_id=0, has_side_effects=True, vmem_limit_bytes=56 * 1024 * 1024
        ),
    )(fetch, choose, live, queries, keys.reshape(-1, BLOCK, keys.shape[1]), values.reshape(-1, BLOCK, values.shape[1]))


def solution(mesh):
    placed = (
        P(("seq", "head"), None),
        P(("seq", "head"), None),
        P(("seq", "head"), None),
        P(),
        P("seq", None),
        P("seq"),
    )
    return jax.shard_map(
        body, mesh=mesh, in_specs=placed, out_specs=P(("seq", "head"), None), check_vma=False
    )
```

```python
import functools
import math

import jax
import jax.numpy as jnp
from jax import lax
from jax.experimental import pallas as pl
from jax.experimental.pallas import tpu as pltpu
from jax.sharding import PartitionSpec as P

MESH = pl.DeviceIdType.MESH
WIDTH = 128
BLOCK = 64
ENTRIES = 16
X, Y, Z = 4, 8, 2
PLANE = Y * Z
GROUP = 8
REPEAT = 5
ROWS = 128
TOKENS = GROUP * ROWS
BLOCKS = TOKENS // BLOCK
QW = REPEAT * WIDTH
Q_FIRST, Q_EVERY = 3, 2
PIECES = GROUP // 2
SCALE = math.log2(math.e) / math.sqrt(WIDTH)


def mirrored(z, i):
    return i + z * (6 + 2 * lax.rem(i, 2) - 2 * i)


def xor3(a, b):
    out = 0
    for bit in (4, 2, 1):
        out = out + bit * lax.rem(lax.rem(a // bit, 2) + lax.rem(b // bit, 2), 2)
    return out


def place(g, t):
    return t if g == 0 or t in (0, Y // 2) else Y // 2 + t


def xor2(a, n):
    return 2 * lax.rem(a // 2 + n // 2, 2) + lax.rem(lax.rem(a, 2) + n % 2, 2)


def kernel(
    fetch_in, choose, live, q_in, k_in, v_in, o_out,
    fetch, q_all, out_buf, items_k, items_v, pick_k, pick_v, got_k, got_v,
    q_send, q_recv, k_send, k_recv, v_send, v_recv,
    z_send, z_recv, f_send, f_recv, y_send, y_recv, x_send, x_recv, w_send, w_recv, o_send, o_recv, local_sem, f_sem,
):
    s = lax.axis_index("seq")
    i = lax.axis_index("head")
    x, y, z = s // PLANE, lax.rem(s // Z, Y), lax.rem(s, Z)
    h = mirrored(z, i)
    own_k, own_v = items_k[0], items_v[0]
    gots = (got_k, got_v)

    def seq_of(ax, ay, az):
        return (ax * Y + ay) * Z + az

    right = (seq_of(x, lax.rem(y + 1, Y), z), i)
    left = (seq_of(x, lax.rem(y + Y - 1, Y), z), i)
    twin = mirrored(1 - z, h)
    across = (seq_of(x, y, 1 - z), twin)

    barrier = pltpu.get_barrier_semaphore()
    for j in range(1, GROUP):
        pl.semaphore_signal(barrier, inc=1, device_id=(s, lax.rem(i + j, GROUP)), device_id_type=MESH)
    for peer in (right, left, across):
        pl.semaphore_signal(barrier, inc=1, device_id=peer, device_id_type=MESH)
    for j in range(1, X):
        for az, ai in ((z, i), (1 - z, twin)):
            pl.semaphore_signal(
                barrier, inc=1, device_id=(seq_of(lax.rem(x + j, X), y, az), ai), device_id_type=MESH
            )

    fetches = [
        pltpu.make_async_copy(fetch_in.at[seq_of(ax, y, az)], fetch.at[ax * Z + az], f_sem.at[ax * Z + az])
        for ax in range(X) for az in range(Z)
    ]
    for copy in fetches:
        copy.start()

    for xo in range(1, X):
        @pl.when(xo > x)
        def _():
            for got in gots:
                got[pl.ds(xo * PLANE * 2, PLANE * 2)] = jnp.zeros((PLANE * 2, BLOCK, WIDTH), jnp.bfloat16)

    for copy in fetches:
        copy.wait()
    pl.semaphore_wait(barrier, GROUP - 1 + 3 + 2 * (X - 1))

    def rows_of(p):
        return pl.ds(pl.multiple_of(p * ROWS, ROWS), ROWS)

    def head_copy(kv, p):
        src, send, recv = ((k_in, k_send, k_recv), (v_in, v_send, v_recv))[kv]
        col = pl.multiple_of(mirrored(z, p) * WIDTH, WIDTH)
        return pltpu.make_async_remote_copy(
            src_ref=src.at[:, :, pl.ds(col, WIDTH)],
            dst_ref=(own_k, own_v)[kv].at[pl.ds(2 * i, 2)],
            send_sem=send.at[p], recv_sem=recv.at[i],
            device_id=(s, p), device_id_type=MESH,
        )

    def head_arrival(kv, p):
        src, send, recv = ((k_in, k_send, k_recv), (v_in, v_send, v_recv))[kv]
        return pltpu.make_async_remote_copy(
            src_ref=src.at[:, :, pl.ds(0, WIDTH)],
            dst_ref=(own_k, own_v)[kv].at[pl.ds(2 * p, 2)],
            send_sem=send.at[p], recv_sem=recv.at[p],
            device_id=(s, p), device_id_type=MESH,
        )

    def q_copy(p):
        col = pl.multiple_of(mirrored(z, p) * QW, WIDTH)
        return pltpu.make_async_remote_copy(
            src_ref=q_in.at[:, pl.ds(col, QW)],
            dst_ref=q_all.at[rows_of(i), :],
            send_sem=q_send.at[p], recv_sem=q_recv.at[i],
            device_id=(s, p), device_id_type=MESH,
        )

    def q_arrival(p):
        return pltpu.make_async_remote_copy(
            src_ref=q_in.at[:, pl.ds(0, QW)],
            dst_ref=q_all.at[rows_of(p), :],
            send_sem=q_send.at[p], recv_sem=q_recv.at[p],
            device_id=(s, p), device_id_type=MESH,
        )

    own_col = pl.multiple_of(h * WIDTH, WIDTH)
    own = [
        pltpu.make_async_copy(k_in.at[:, :, pl.ds(own_col, WIDTH)], own_k.at[pl.ds(2 * i, 2)], local_sem.at[0]),
        pltpu.make_async_copy(v_in.at[:, :, pl.ds(own_col, WIDTH)], own_v.at[pl.ds(2 * i, 2)], local_sem.at[1]),
        pltpu.make_async_copy(
            q_in.at[:, pl.ds(pl.multiple_of(h * QW, WIDTH), QW)], q_all.at[rows_of(i), :], local_sem.at[2]
        ),
    ]
    for kv in range(2):
        for j in (4, 3, 5, 2, 6, 1, 7):
            head_copy(kv, lax.rem(i + j, GROUP)).start()
        own[kv].start()
    own[2].start()

    def item(kv, g, t, other):
        return items_v[place(g, t)] if kv else items_k[other + 2 * place(g, t)]

    def ring_copy(g, t, other, kv):
        src, dst = item(kv, g, t, other), item(kv, g, t + 1, other)
        if t == Y // 2 - 1:
            part = pl.ds(g * (BLOCKS // 2), BLOCKS // 2)
            src, dst = src.at[part], dst.at[part]
        return pltpu.make_async_remote_copy(
            src_ref=src, dst_ref=dst,
            send_sem=y_send.at[g, t, other, kv], recv_sem=y_recv.at[g, t, other, kv],
            device_id=(right, left)[g], device_id_type=MESH,
        )

    def piece(n):
        return xor2(i // 2, n)

    def first_copy(g, kv, c):
        part = pl.ds(4 * c, 4)
        return pltpu.make_async_remote_copy(
            src_ref=item(kv, g, 0, 0).at[part], dst_ref=item(kv, g, 1, 0).at[part],
            send_sem=f_send.at[g, kv, c], recv_sem=f_recv.at[g, kv, c],
            device_id=(right, left)[g], device_id_type=MESH,
        )

    def ring_wait(g, t, other, kv):
        if t == 0 and other == 0:
            for c in range(PIECES):
                first_copy(g, kv, c).wait_recv()
        else:
            ring_copy(g, t, other, kv).wait_recv()

    def z_copy(kv):
        return pltpu.make_async_remote_copy(
            src_ref=item(kv, 0, 0, 0), dst_ref=item(kv, 0, 0, 1), send_sem=z_send.at[kv], recv_sem=z_recv.at[kv],
            device_id=across, device_id_type=MESH,
        )

    def wanted(ax, az, o, e):
        return fetch[ax * Z + az, e, x * PLANE + o]

    def x_copy(dx, o):
        return pltpu.make_async_remote_copy(
            src_ref=pick_k.at[dx - 1, pl.ds(o * 2, 2)],
            dst_ref=got_k.at[pl.ds((x * PLANE + o) * 2, 2)],
            send_sem=x_send.at[dx - 1, o], recv_sem=x_recv.at[x, o],
            device_id=(seq_of(lax.rem(x + dx, X), y, z), i), device_id_type=MESH,
        )

    def x_arrival(xo, o):
        return pltpu.make_async_remote_copy(
            src_ref=pick_k.at[0, pl.ds(o * 2, 2)],
            dst_ref=got_k.at[pl.ds((xo * PLANE + o) * 2, 2)],
            send_sem=x_send.at[0, o], recv_sem=x_recv.at[xo, o],
            device_id=(seq_of(xo, y, z), i), device_id_type=MESH,
        )

    def w_copy(dx, dz, oy):
        return pltpu.make_async_remote_copy(
            src_ref=pick_v.at[dx * Z + dz, pl.ds(oy * 2, 2)],
            dst_ref=got_v.at[pl.ds((x * PLANE + oy * Z + z) * 2, 2)],
            send_sem=w_send.at[dx * Z + dz, oy], recv_sem=w_recv.at[x, oy * Z + z],
            device_id=(seq_of(lax.rem(x + dx, X), y, 1 - z if dz else z), twin if dz else i), device_id_type=MESH,
        )

    def w_arrival(xo, o):
        return pltpu.make_async_remote_copy(
            src_ref=pick_v.at[0, pl.ds(0, 2)],
            dst_ref=got_v.at[pl.ds((xo * PLANE + o) * 2, 2)],
            send_sem=w_send.at[0, 0], recv_sem=w_recv.at[xo, o],
            device_id=across, device_id_type=MESH,
        )

    def select(kv, src, oy, o):
        for e in range(2):
            gots[kv][(x * PLANE + o) * 2 + e] = src[wanted(x, z, o, e)]
        for dx in range(X):
            @pl.when(x + dx < X)
            def _():
                for e in range(2):
                    if kv == 0 and dx > 0:
                        pick_k[dx - 1, o * 2 + e] = src[wanted(x + dx, z, o, e)]
                    if kv == 1:
                        pick_v[dx * Z + 1, oy * 2 + e] = src[wanted(x + dx, 1 - z, o, e)]
                        if dx > 0:
                            pick_v[dx * Z, oy * 2 + e] = src[wanted(x + dx, z, o, e)]

    def forward(kv, oy, o):
        for dx in range(X):
            @pl.when(x + dx < X)
            def _():
                if kv == 1:
                    w_copy(dx, 1, oy).start()
                if dx > 0:
                    (x_copy(dx, o) if kv == 0 else w_copy(dx, 0, oy)).start()

    pending = []
    q_order = [4, 3, 5, 2, 6, 1, 7]

    def pick(kv, g, t, other):
        oy = lax.rem(y + (Y - t if g == 0 else t), Y)
        o = oy * Z + (1 - z if other else z)
        select(kv, item(kv, g, t, other), oy, o)
        pending.append((kv, oy, o))
        forward(*pending[-1])
        if len(pending) >= Q_FIRST and (len(pending) - Q_FIRST) % Q_EVERY == 0 and q_order:
            q_copy(lax.rem(i + q_order.pop(0), GROUP)).start()

    for kv in range(2):
        own[kv].wait()
        for n in range(PIECES):
            c = piece(n)
            for core in range(2):
                p = 2 * c + core
                if n > 0:
                    head_arrival(kv, p).wait_recv()
                else:
                    @pl.when(p != i)
                    def _():
                        head_arrival(kv, p).wait_recv()
            first_copy(0, kv, c).start()
            first_copy(1, kv, c).start()
        if kv == 0:
            z_copy(0).start()
        pick(kv, 0, 0, 0)
    z_copy(0).wait_recv()
    ring_copy(0, 0, 1, 0).start()
    ring_copy(1, 0, 1, 0).start()
    pick(0, 0, 0, 1)
    half = Y // 2
    travels = ((0, 0), (1, 0), (0, 1))
    for t in range(1, half + 1):
        for kv, other in travels:
            for g in range(2):
                ring_wait(g, t - 1, other, kv)
                if t < half:
                    ring_copy(g, t, other, kv).start()
                    pick(kv, g, t, other)
            if t == half:
                pick(kv, 0, t, other)
    for j in q_order:
        q_copy(lax.rem(i + j, GROUP)).start()

    own[2].wait()
    for j in range(1, GROUP):
        q_arrival(lax.rem(i + j, GROUP)).wait_recv()
    for xo in range(X):
        @pl.when(xo < x)
        def _():
            def one(o, carry):
                x_arrival(xo, o).wait_recv()
                w_arrival(xo, o).wait_recv()
                return carry
            lax.fori_loop(0, PLANE, one, 0)
    for oy in range(Y):
        w_arrival(x, oy * Z + 1 - z).wait_recv()

    def out_copy(p, half_block):
        return pltpu.make_async_remote_copy(
            src_ref=out_buf.at[pl.ds(pl.multiple_of((p * 2 + half_block) * BLOCK, BLOCK), BLOCK), :],
            dst_ref=o_out.at[pl.ds(half_block * BLOCK, BLOCK), pl.ds(pl.multiple_of(h * QW, WIDTH), QW)],
            send_sem=o_send.at[p, half_block], recv_sem=o_recv.at[i, half_block],
            device_id=(s, p), device_id_type=MESH,
        )

    def out_arrival(p, half_block):
        return pltpu.make_async_remote_copy(
            src_ref=out_buf.at[pl.ds(half_block * BLOCK, BLOCK), :],
            dst_ref=o_out.at[
                pl.ds(half_block * BLOCK, BLOCK), pl.ds(pl.multiple_of(mirrored(z, p) * QW, WIDTH), QW)
            ],
            send_sem=o_send.at[p, half_block], recv_sem=o_recv.at[p, half_block],
            device_id=(s, p), device_id_type=MESH,
        )

    contract_last = (((1,), (1,)), ((), ()))
    contract = (((1,), (0,)), ((), ()))

    def attend(b):
        first = pl.multiple_of(b * BLOCK, BLOCK)
        q_rows = q_all[pl.ds(first, BLOCK), :]
        q = jnp.concatenate([q_rows[:, g * WIDTH:(g + 1) * WIDTH] for g in range(REPEAT)], axis=0)
        slots = [choose[b, e] for e in range(ENTRIES)]
        k_listed = jnp.concatenate([got_k[slot] for slot in slots], axis=0)
        k_own = own_k[b]
        far = lax.dot_general(q, k_listed, contract_last, preferred_element_type=jnp.float32)
        near = lax.dot_general(q, k_own, contract_last, preferred_element_type=jnp.float32)
        column = lax.broadcasted_iota(jnp.int32, (1, ENTRIES * BLOCK), 1)
        far = jnp.where(column < live[b] * BLOCK, far, -jnp.inf)
        row = lax.rem(lax.broadcasted_iota(jnp.int32, (REPEAT * BLOCK, BLOCK), 0), BLOCK)
        near = jnp.where(lax.broadcasted_iota(jnp.int32, (REPEAT * BLOCK, BLOCK), 1) <= row, near, -jnp.inf)
        highest = jnp.maximum(jnp.max(far, axis=1, keepdims=True), jnp.max(near, axis=1, keepdims=True)) * SCALE
        far = jnp.exp2(far * SCALE - highest)
        near = jnp.exp2(near * SCALE - highest)
        totals = jnp.sum(far, axis=1, keepdims=True) + jnp.sum(near, axis=1, keepdims=True)
        v_listed = jnp.concatenate([got_v[slot] for slot in slots], axis=0)
        v_own = own_v[b]
        mixed = lax.dot_general(far.astype(jnp.bfloat16), v_listed, contract, preferred_element_type=jnp.float32)
        mixed += lax.dot_general(near.astype(jnp.bfloat16), v_own, contract, preferred_element_type=jnp.float32)
        result = (mixed / totals).astype(jnp.bfloat16)
        for g in range(REPEAT):
            out_buf[pl.ds(first, BLOCK), g * WIDTH:(g + 1) * WIDTH] = result[g * BLOCK:(g + 1) * BLOCK]

    def one_pair(t, carry):
        p = xor3(7 - i, t)
        for half_block in range(2):
            attend(p * 2 + half_block)

            @pl.when(t < GROUP - 1)
            def _():
                out_copy(p, half_block).start()
        return carry

    lax.fori_loop(0, GROUP, one_pair, 0)
    back = pltpu.make_async_copy(
        out_buf.at[rows_of(i), :], o_out.at[:, pl.ds(pl.multiple_of(h * QW, WIDTH), QW)], local_sem.at[3]
    )
    back.start()

    for j in range(1, GROUP):
        p = lax.rem(i + j, GROUP)
        for kv in range(2):
            head_copy(kv, p).wait_send()
        q_copy(p).wait_send()
        for half_block in range(2):
            out_copy(p, half_block).wait_send()
    z_copy(0).wait_send()
    for t in range(half):
        for kv, other in travels:
            for g in range(2):
                if t == 0 and other == 0:
                    for c in range(PIECES):
                        first_copy(g, kv, c).wait_send()
                else:
                    ring_copy(g, t, other, kv).wait_send()
    for dx in range(X):
        @pl.when(x + dx < X)
        def _():
            def one(oy, carry):
                w_copy(dx, 1, oy).wait_send()
                if dx > 0:
                    w_copy(dx, 0, oy).wait_send()
                    x_copy(dx, oy * Z).wait_send()
                    x_copy(dx, oy * Z + 1).wait_send()
                return carry
            lax.fori_loop(0, Y, one, 0)
    back.wait()
    for j in range(1, GROUP):
        p = lax.rem(i + j, GROUP)
        for half_block in range(2):
            out_arrival(p, half_block).wait_recv()


def body(queries, keys, values, fetch_list, choose, live):
    fetch = fetch_list.transpose(0, 2, 1)
    dma = pltpu.SemaphoreType.DMA
    half = Y // 2
    smem = pl.BlockSpec(memory_space=pltpu.SMEM)
    anywhere = pl.BlockSpec(memory_space=pl.ANY)
    bf16 = jnp.bfloat16
    return pl.pallas_call(
        kernel,
        out_shape=jax.ShapeDtypeStruct(queries.shape, bf16),
        in_specs=[anywhere, smem, smem, anywhere, anywhere, anywhere],
        out_specs=anywhere,
        scratch_shapes=[
            pltpu.SMEM((X * Z, 2, X * PLANE), jnp.int32),
            pltpu.VMEM((TOKENS, QW), bf16),
            pltpu.VMEM((TOKENS, QW), bf16),
            [pltpu.VMEM((BLOCKS, BLOCK, WIDTH), bf16)] * PLANE,
            [pltpu.VMEM((BLOCKS, BLOCK, WIDTH), bf16)] * Y,
            pltpu.VMEM((X - 1, PLANE * 2, BLOCK, WIDTH), bf16),
            pltpu.VMEM((X * Z, Y * 2, BLOCK, WIDTH), bf16),
            pltpu.VMEM((X * PLANE * 2, BLOCK, WIDTH), bf16),
            pltpu.VMEM((X * PLANE * 2, BLOCK, WIDTH), bf16),
            dma((GROUP,)), dma((GROUP,)), dma((GROUP,)), dma((GROUP,)), dma((GROUP,)), dma((GROUP,)),
            dma((1,)), dma((1,)),
            dma((2, 2, PIECES)), dma((2, 2, PIECES)),
            dma((2, half, 2, 2)), dma((2, half, 2, 2)),
            dma((X - 1, PLANE)), dma((X, PLANE)),
            dma((X * Z, Y)), dma((X, PLANE)),
            dma((GROUP, 2)), dma((GROUP, 2)),
            dma((4,)), dma((X * Z,)),
        ],
        compiler_params=pltpu.CompilerParams(
            collective_id=0, has_side_effects=True, vmem_limit_bytes=56 * 1024 * 1024
        ),
    )(fetch, choose, live, queries, keys.reshape(-1, BLOCK, keys.shape[1]), values.reshape(-1, BLOCK, values.shape[1]))


def solution(mesh):
    placed = (
        P(("seq", "head"), None),
        P(("seq", "head"), None),
        P(("seq", "head"), None),
        P(),
        P("seq", None),
        P("seq"),
    )
    return jax.shard_map(
        body, mesh=mesh, in_specs=placed, out_specs=P(("seq", "head"), None), check_vma=False
    )
```

```python
import functools
import math

import jax
import jax.numpy as jnp
from jax import lax
from jax.experimental import pallas as pl
from jax.experimental.pallas import tpu as pltpu
from jax.sharding import PartitionSpec as P

MESH = pl.DeviceIdType.MESH
WIDTH = 128
BLOCK = 64
ENTRIES = 16
X, Y, Z = 4, 8, 2
PLANE = Y * Z
GROUP = 8
REPEAT = 5
ROWS = 128
TOKENS = GROUP * ROWS
BLOCKS = TOKENS // BLOCK
QW = REPEAT * WIDTH
Q_FIRST, Q_EVERY = 3, 2
PIECES = GROUP // 2
SCALE = math.log2(math.e) / math.sqrt(WIDTH)


def mirrored(z, i):
    return i + z * (6 + 2 * lax.rem(i, 2) - 2 * i)


def xor3(a, b):
    out = 0
    for bit in (4, 2, 1):
        out = out + bit * lax.rem(lax.rem(a // bit, 2) + lax.rem(b // bit, 2), 2)
    return out


def place(g, t):
    return t if g == 0 or t in (0, Y // 2) else Y // 2 + t


def xor2(a, n):
    return 2 * lax.rem(a // 2 + n // 2, 2) + lax.rem(lax.rem(a, 2) + n % 2, 2)


def kernel(
    fetch_in, choose, live, q_in, k_in, v_in, o_out,
    fetch, q_all, out_buf, items_k, items_v, pick_k, pick_v, got_k, got_v,
    q_send, q_recv, k_send, k_recv, v_send, v_recv,
    z_send, z_recv, f_send, f_recv, y_send, y_recv, x_send, x_recv, w_send, w_recv, o_send, o_recv, local_sem, f_sem,
):
    s = lax.axis_index("seq")
    i = lax.axis_index("head")
    x, y, z = s // PLANE, lax.rem(s // Z, Y), lax.rem(s, Z)
    h = mirrored(z, i)
    own_k, own_v = items_k[0], items_v[0]
    gots = (got_k, got_v)

    def seq_of(ax, ay, az):
        return (ax * Y + ay) * Z + az

    right = (seq_of(x, lax.rem(y + 1, Y), z), i)
    left = (seq_of(x, lax.rem(y + Y - 1, Y), z), i)
    twin = mirrored(1 - z, h)
    across = (seq_of(x, y, 1 - z), twin)

    barrier = pltpu.get_barrier_semaphore()
    for j in range(1, GROUP):
        pl.semaphore_signal(barrier, inc=1, device_id=(s, lax.rem(i + j, GROUP)), device_id_type=MESH)
    for peer in (right, left, across):
        pl.semaphore_signal(barrier, inc=1, device_id=peer, device_id_type=MESH)
    for j in range(1, X):
        for az, ai in ((z, i), (1 - z, twin)):
            pl.semaphore_signal(
                barrier, inc=1, device_id=(seq_of(lax.rem(x + j, X), y, az), ai), device_id_type=MESH
            )

    fetches = [
        pltpu.make_async_copy(fetch_in.at[seq_of(ax, y, az)], fetch.at[ax * Z + az], f_sem.at[ax * Z + az])
        for ax in range(X) for az in range(Z)
    ]
    for copy in fetches:
        copy.start()

    for xo in range(1, X):
        @pl.when(xo > x)
        def _():
            for got in gots:
                got[pl.ds(xo * PLANE * 2, PLANE * 2)] = jnp.zeros((PLANE * 2, BLOCK, WIDTH), jnp.bfloat16)

    for copy in fetches:
        copy.wait()
    pl.semaphore_wait(barrier, GROUP - 1 + 3 + 2 * (X - 1))

    def rows_of(p):
        return pl.ds(pl.multiple_of(p * ROWS, ROWS), ROWS)

    def head_copy(kv, p):
        src, send, recv = ((k_in, k_send, k_recv), (v_in, v_send, v_recv))[kv]
        col = pl.multiple_of(mirrored(z, p) * WIDTH, WIDTH)
        return pltpu.make_async_remote_copy(
            src_ref=src.at[:, :, pl.ds(col, WIDTH)],
            dst_ref=(own_k, own_v)[kv].at[pl.ds(2 * i, 2)],
            send_sem=send.at[p], recv_sem=recv.at[i],
            device_id=(s, p), device_id_type=MESH,
        )

    def head_arrival(kv, p):
        src, send, recv = ((k_in, k_send, k_recv), (v_in, v_send, v_recv))[kv]
        return pltpu.make_async_remote_copy(
            src_ref=src.at[:, :, pl.ds(0, WIDTH)],
            dst_ref=(own_k, own_v)[kv].at[pl.ds(2 * p, 2)],
            send_sem=send.at[p], recv_sem=recv.at[p],
            device_id=(s, p), device_id_type=MESH,
        )

    def q_copy(p):
        col = pl.multiple_of(mirrored(z, p) * QW, WIDTH)
        return pltpu.make_async_remote_copy(
            src_ref=q_in.at[:, pl.ds(col, QW)],
            dst_ref=q_all.at[rows_of(i), :],
            send_sem=q_send.at[p], recv_sem=q_recv.at[i],
            device_id=(s, p), device_id_type=MESH,
        )

    def q_arrival(p):
        return pltpu.make_async_remote_copy(
            src_ref=q_in.at[:, pl.ds(0, QW)],
            dst_ref=q_all.at[rows_of(p), :],
            send_sem=q_send.at[p], recv_sem=q_recv.at[p],
            device_id=(s, p), device_id_type=MESH,
        )

    own_col = pl.multiple_of(h * WIDTH, WIDTH)
    own = [
        pltpu.make_async_copy(k_in.at[:, :, pl.ds(own_col, WIDTH)], own_k.at[pl.ds(2 * i, 2)], local_sem.at[0]),
        pltpu.make_async_copy(v_in.at[:, :, pl.ds(own_col, WIDTH)], own_v.at[pl.ds(2 * i, 2)], local_sem.at[1]),
        pltpu.make_async_copy(
            q_in.at[:, pl.ds(pl.multiple_of(h * QW, WIDTH), QW)], q_all.at[rows_of(i), :], local_sem.at[2]
        ),
    ]
    for kv in range(2):
        for j in (4, 3, 5, 2, 6, 1, 7):
            head_copy(kv, lax.rem(i + j, GROUP)).start()
        own[kv].start()
    own[2].start()

    def item(kv, g, t, other):
        return items_v[place(g, t)] if kv else items_k[other + 2 * place(g, t)]

    def ring_copy(g, t, other, kv):
        src, dst = item(kv, g, t, other), item(kv, g, t + 1, other)
        if t == Y // 2 - 1:
            part = pl.ds(g * (BLOCKS // 2), BLOCKS // 2)
            src, dst = src.at[part], dst.at[part]
        return pltpu.make_async_remote_copy(
            src_ref=src, dst_ref=dst,
            send_sem=y_send.at[g, t, other, kv], recv_sem=y_recv.at[g, t, other, kv],
            device_id=(right, left)[g], device_id_type=MESH,
        )

    def piece(n):
        return xor2(i // 2, n)

    def first_copy(g, kv, c):
        part = pl.ds(4 * c, 4)
        return pltpu.make_async_remote_copy(
            src_ref=item(kv, g, 0, 0).at[part], dst_ref=item(kv, g, 1, 0).at[part],
            send_sem=f_send.at[g, kv, c], recv_sem=f_recv.at[g, kv, c],
            device_id=(right, left)[g], device_id_type=MESH,
        )

    def ring_wait(g, t, other, kv):
        if t == 0 and other == 0:
            for c in range(PIECES):
                first_copy(g, kv, c).wait_recv()
        else:
            ring_copy(g, t, other, kv).wait_recv()

    def z_copy(kv):
        return pltpu.make_async_remote_copy(
            src_ref=item(kv, 0, 0, 0), dst_ref=item(kv, 0, 0, 1), send_sem=z_send.at[kv], recv_sem=z_recv.at[kv],
            device_id=across, device_id_type=MESH,
        )

    def wanted(ax, az, o, e):
        return fetch[ax * Z + az, e, x * PLANE + o]

    def x_copy(dx, o):
        return pltpu.make_async_remote_copy(
            src_ref=pick_k.at[dx - 1, pl.ds(o * 2, 2)],
            dst_ref=got_k.at[pl.ds((x * PLANE + o) * 2, 2)],
            send_sem=x_send.at[dx - 1, o], recv_sem=x_recv.at[x, o],
            device_id=(seq_of(lax.rem(x + dx, X), y, z), i), device_id_type=MESH,
        )

    def x_arrival(xo, o):
        return pltpu.make_async_remote_copy(
            src_ref=pick_k.at[0, pl.ds(o * 2, 2)],
            dst_ref=got_k.at[pl.ds((xo * PLANE + o) * 2, 2)],
            send_sem=x_send.at[0, o], recv_sem=x_recv.at[xo, o],
            device_id=(seq_of(xo, y, z), i), device_id_type=MESH,
        )

    def w_copy(dx, dz, oy):
        return pltpu.make_async_remote_copy(
            src_ref=pick_v.at[dx * Z + dz, pl.ds(oy * 2, 2)],
            dst_ref=got_v.at[pl.ds((x * PLANE + oy * Z + z) * 2, 2)],
            send_sem=w_send.at[dx * Z + dz, oy], recv_sem=w_recv.at[x, oy * Z + z],
            device_id=(seq_of(lax.rem(x + dx, X), y, 1 - z if dz else z), twin if dz else i), device_id_type=MESH,
        )

    def w_arrival(xo, o):
        return pltpu.make_async_remote_copy(
            src_ref=pick_v.at[0, pl.ds(0, 2)],
            dst_ref=got_v.at[pl.ds((xo * PLANE + o) * 2, 2)],
            send_sem=w_send.at[0, 0], recv_sem=w_recv.at[xo, o],
            device_id=across, device_id_type=MESH,
        )

    def select(kv, src, oy, o):
        for e in range(2):
            gots[kv][(x * PLANE + o) * 2 + e] = src[wanted(x, z, o, e)]
        for dx in range(X):
            @pl.when(x + dx < X)
            def _():
                for e in range(2):
                    if kv == 0 and dx > 0:
                        pick_k[dx - 1, o * 2 + e] = src[wanted(x + dx, z, o, e)]
                    if kv == 1:
                        pick_v[dx * Z + 1, oy * 2 + e] = src[wanted(x + dx, 1 - z, o, e)]
                        if dx > 0:
                            pick_v[dx * Z, oy * 2 + e] = src[wanted(x + dx, z, o, e)]

    def forward(kv, oy, o):
        for dx in range(X):
            @pl.when(x + dx < X)
            def _():
                if kv == 1:
                    w_copy(dx, 1, oy).start()
                if dx > 0:
                    (x_copy(dx, o) if kv == 0 else w_copy(dx, 0, oy)).start()

    pending = []
    q_order = [4, 3, 5, 2, 6, 1, 7]

    def pick(kv, g, t, other):
        oy = lax.rem(y + (Y - t if g == 0 else t), Y)
        o = oy * Z + (1 - z if other else z)
        select(kv, item(kv, g, t, other), oy, o)
        pending.append((kv, oy, o))
        forward(*pending[-1])
        if len(pending) >= Q_FIRST and (len(pending) - Q_FIRST) % Q_EVERY == 0 and q_order:
            q_copy(lax.rem(i + q_order.pop(0), GROUP)).start()

    for kv in range(2):
        own[kv].wait()
        for n in range(PIECES):
            c = piece(n)
            for core in range(2):
                p = 2 * c + core
                if n > 0:
                    head_arrival(kv, p).wait_recv()
                else:
                    @pl.when(p != i)
                    def _():
                        head_arrival(kv, p).wait_recv()
            first_copy(0, kv, c).start()
            first_copy(1, kv, c).start()
        if kv == 0:
            z_copy(0).start()
        pick(kv, 0, 0, 0)
    half = Y // 2
    travels = ((0, 0), (1, 0), (0, 1))

    def ring_step(t, kv, other):
        for g in range(2):
            ring_wait(g, t - 1, other, kv)
            if t < half:
                ring_copy(g, t, other, kv).start()
                pick(kv, g, t, other)
        if t == half:
            pick(kv, 0, t, other)

    for t in range(1, half + 2):
        if t <= half:
            ring_step(t, 0, 0)
            ring_step(t, 1, 0)
        if t == 1:
            z_copy(0).wait_recv()
            ring_copy(0, 0, 1, 0).start()
            ring_copy(1, 0, 1, 0).start()
            pick(0, 0, 0, 1)
        else:
            ring_step(t - 1, 0, 1)
    for j in q_order:
        q_copy(lax.rem(i + j, GROUP)).start()

    own[2].wait()
    for j in range(1, GROUP):
        q_arrival(lax.rem(i + j, GROUP)).wait_recv()
    for xo in range(X):
        @pl.when(xo < x)
        def _():
            def one(o, carry):
                x_arrival(xo, o).wait_recv()
                w_arrival(xo, o).wait_recv()
                return carry
            lax.fori_loop(0, PLANE, one, 0)
    for oy in range(Y):
        w_arrival(x, oy * Z + 1 - z).wait_recv()

    def out_copy(p, half_block):
        return pltpu.make_async_remote_copy(
            src_ref=out_buf.at[pl.ds(pl.multiple_of((p * 2 + half_block) * BLOCK, BLOCK), BLOCK), :],
            dst_ref=o_out.at[pl.ds(half_block * BLOCK, BLOCK), pl.ds(pl.multiple_of(h * QW, WIDTH), QW)],
            send_sem=o_send.at[p, half_block], recv_sem=o_recv.at[i, half_block],
            device_id=(s, p), device_id_type=MESH,
        )

    def out_arrival(p, half_block):
        return pltpu.make_async_remote_copy(
            src_ref=out_buf.at[pl.ds(half_block * BLOCK, BLOCK), :],
            dst_ref=o_out.at[
                pl.ds(half_block * BLOCK, BLOCK), pl.ds(pl.multiple_of(mirrored(z, p) * QW, WIDTH), QW)
            ],
            send_sem=o_send.at[p, half_block], recv_sem=o_recv.at[p, half_block],
            device_id=(s, p), device_id_type=MESH,
        )

    contract_last = (((1,), (1,)), ((), ()))
    contract = (((1,), (0,)), ((), ()))

    def attend(b):
        first = pl.multiple_of(b * BLOCK, BLOCK)
        q_rows = q_all[pl.ds(first, BLOCK), :]
        q = jnp.concatenate([q_rows[:, g * WIDTH:(g + 1) * WIDTH] for g in range(REPEAT)], axis=0)
        slots = [choose[b, e] for e in range(ENTRIES)]
        k_listed = jnp.concatenate([got_k[slot] for slot in slots], axis=0)
        k_own = own_k[b]
        far = lax.dot_general(q, k_listed, contract_last, preferred_element_type=jnp.float32)
        near = lax.dot_general(q, k_own, contract_last, preferred_element_type=jnp.float32)
        column = lax.broadcasted_iota(jnp.int32, (1, ENTRIES * BLOCK), 1)
        far = jnp.where(column < live[b] * BLOCK, far, -jnp.inf)
        row = lax.rem(lax.broadcasted_iota(jnp.int32, (REPEAT * BLOCK, BLOCK), 0), BLOCK)
        near = jnp.where(lax.broadcasted_iota(jnp.int32, (REPEAT * BLOCK, BLOCK), 1) <= row, near, -jnp.inf)
        highest = jnp.maximum(jnp.max(far, axis=1, keepdims=True), jnp.max(near, axis=1, keepdims=True)) * SCALE
        far = jnp.exp2(far * SCALE - highest)
        near = jnp.exp2(near * SCALE - highest)
        totals = jnp.sum(far, axis=1, keepdims=True) + jnp.sum(near, axis=1, keepdims=True)
        v_listed = jnp.concatenate([got_v[slot] for slot in slots], axis=0)
        v_own = own_v[b]
        mixed = lax.dot_general(far.astype(jnp.bfloat16), v_listed, contract, preferred_element_type=jnp.float32)
        mixed += lax.dot_general(near.astype(jnp.bfloat16), v_own, contract, preferred_element_type=jnp.float32)
        result = (mixed / totals).astype(jnp.bfloat16)
        for g in range(REPEAT):
            out_buf[pl.ds(first, BLOCK), g * WIDTH:(g + 1) * WIDTH] = result[g * BLOCK:(g + 1) * BLOCK]

    def one_pair(t, carry):
        p = xor3(7 - i, t)
        for half_block in range(2):
            attend(p * 2 + half_block)

            @pl.when(t < GROUP - 1)
            def _():
                out_copy(p, half_block).start()
        return carry

    lax.fori_loop(0, GROUP, one_pair, 0)
    back = pltpu.make_async_copy(
        out_buf.at[rows_of(i), :], o_out.at[:, pl.ds(pl.multiple_of(h * QW, WIDTH), QW)], local_sem.at[3]
    )
    back.start()

    for j in range(1, GROUP):
        p = lax.rem(i + j, GROUP)
        for kv in range(2):
            head_copy(kv, p).wait_send()
        q_copy(p).wait_send()
        for half_block in range(2):
            out_copy(p, half_block).wait_send()
    z_copy(0).wait_send()
    for t in range(half):
        for kv, other in travels:
            for g in range(2):
                if t == 0 and other == 0:
                    for c in range(PIECES):
                        first_copy(g, kv, c).wait_send()
                else:
                    ring_copy(g, t, other, kv).wait_send()
    for dx in range(X):
        @pl.when(x + dx < X)
        def _():
            def one(oy, carry):
                w_copy(dx, 1, oy).wait_send()
                if dx > 0:
                    w_copy(dx, 0, oy).wait_send()
                    x_copy(dx, oy * Z).wait_send()
                    x_copy(dx, oy * Z + 1).wait_send()
                return carry
            lax.fori_loop(0, Y, one, 0)
    back.wait()
    for j in range(1, GROUP):
        p = lax.rem(i + j, GROUP)
        for half_block in range(2):
            out_arrival(p, half_block).wait_recv()


def body(queries, keys, values, fetch_list, choose, live):
    fetch = fetch_list.transpose(0, 2, 1)
    dma = pltpu.SemaphoreType.DMA
    half = Y // 2
    smem = pl.BlockSpec(memory_space=pltpu.SMEM)
    anywhere = pl.BlockSpec(memory_space=pl.ANY)
    bf16 = jnp.bfloat16
    return pl.pallas_call(
        kernel,
        out_shape=jax.ShapeDtypeStruct(queries.shape, bf16),
        in_specs=[anywhere, smem, smem, anywhere, anywhere, anywhere],
        out_specs=anywhere,
        scratch_shapes=[
            pltpu.SMEM((X * Z, 2, X * PLANE), jnp.int32),
            pltpu.VMEM((TOKENS, QW), bf16),
            pltpu.VMEM((TOKENS, QW), bf16),
            [pltpu.VMEM((BLOCKS, BLOCK, WIDTH), bf16)] * PLANE,
            [pltpu.VMEM((BLOCKS, BLOCK, WIDTH), bf16)] * Y,
            pltpu.VMEM((X - 1, PLANE * 2, BLOCK, WIDTH), bf16),
            pltpu.VMEM((X * Z, Y * 2, BLOCK, WIDTH), bf16),
            pltpu.VMEM((X * PLANE * 2, BLOCK, WIDTH), bf16),
            pltpu.VMEM((X * PLANE * 2, BLOCK, WIDTH), bf16),
            dma((GROUP,)), dma((GROUP,)), dma((GROUP,)), dma((GROUP,)), dma((GROUP,)), dma((GROUP,)),
            dma((1,)), dma((1,)),
            dma((2, 2, PIECES)), dma((2, 2, PIECES)),
            dma((2, half, 2, 2)), dma((2, half, 2, 2)),
            dma((X - 1, PLANE)), dma((X, PLANE)),
            dma((X * Z, Y)), dma((X, PLANE)),
            dma((GROUP, 2)), dma((GROUP, 2)),
            dma((4,)), dma((X * Z,)),
        ],
        compiler_params=pltpu.CompilerParams(
            collective_id=0, has_side_effects=True, vmem_limit_bytes=56 * 1024 * 1024
        ),
    )(fetch, choose, live, queries, keys.reshape(-1, BLOCK, keys.shape[1]), values.reshape(-1, BLOCK, values.shape[1]))


def solution(mesh):
    placed = (
        P(("seq", "head"), None),
        P(("seq", "head"), None),
        P(("seq", "head"), None),
        P(),
        P("seq", None),
        P("seq"),
    )
    return jax.shard_map(
        body, mesh=mesh, in_specs=placed, out_specs=P(("seq", "head"), None), check_vma=False
    )
```
